32 devices in a mesh: seq: 8 (over z, y), head: 4 (over x, core).
Axes of the slice: x: 2, y: 2, z: 4, core: 2. Of those that a mesh axis runs over, the one named last changes fastest.
Arguments:
- signal: bfloat16 [2048, 2048], P('seq', 'head'), may hold values from -6 to 6
- gate: bfloat16 [2048, 2048], P('seq', 'head'), may hold values from -6 to 6
- skip: float32 [2048], P('head'), may hold values from -4 to 4
- w_first: float32 [33, 64], replicated, may hold values from -1 to 1
- b_first: float32 [64], replicated, may hold values from -3.140625 to 3.140625
- freq: float32 [64], replicated, may hold values from 0.5 to 2
- w_mid: float32 [64, 64], replicated, may hold values from -0.75 to 0.75
- w_last: float32 [64, 2048], P(None, 'head'), may hold values from -0.046875 to 0.046875
- rate: float32 [2048], P('head'), may hold values from 0.00014648438 to 0.08
- out_w: bfloat16 [2048, 2048], P('head'), may hold values from -0.125 to 0.125
Outputs:
- output: bfloat16 [2048, 2048], P('seq', 'head')
The draws below stay inside these ranges and needn't reach their ends.
All inputs are finite; a program needn't handle non-finite values.
Results may differ from the reference program's by a relative error of at most 0.0054.
Values may be sent and summed in bfloat16 or wider, within the bound.
No kernel may reach another device: no remote copies, remote signals or barrier semaphores. Data moves between devices by JAX's collectives and lax.ppermute only.
A program may use at most 64 MiB of HBM per device.

```python
import math
import jax
import jax.numpy as jnp
from jax import lax

D = 2048
K = 2048
FH = 64
BANDS = 16
E = 33
LENGTH = 2048


def draw_w_first(key, part):
    own_key = jax.random.fold_in(key, 101)
    return jax.random.uniform(own_key, (E, FH), jnp.float32, -1.0, 1.0)


def draw_w_mid(key, part):
    own_key = jax.random.fold_in(key, 202)
    return jax.random.uniform(own_key, (FH, FH), jnp.float32, -0.75, 0.75)


def block_scale(key, extent, cuts, low, high):
    level, own = 1.0, jax.random.fold_in(key, 6)
    for dim, blocks in cuts:
        heights = jnp.exp(jax.random.uniform(jax.random.fold_in(own, dim), (blocks,), jnp.float32, low / len(cuts), high / len(cuts)))
        level = level * jnp.repeat(heights, extent[dim] // blocks).reshape([-1 if axis == dim else 1 for axis in range(len(extent))])
    return level


def bell_draw(key, extent, deviation, reach, pieces=(), dtype=jnp.bfloat16):
    array = deviation * jax.random.normal(key, extent, jnp.float32)
    if pieces:
        array = array * block_scale(key, extent, pieces, -0.22, 0.18)
    return jnp.clip(array, -reach, reach).astype(dtype)


def setup_inputs(seed: int = 0) -> dict:
    streams_of = jax.random.split(jax.random.key(seed), 11)
    return {
        "signal": bell_draw(streams_of[0], (LENGTH, D), 1.0, 6.0, ((0, 8), (1, 4))),
        "gate": bell_draw(streams_of[1], (LENGTH, D), 1.0, 6.0, ((0, 8), (1, 4))),
        "skip": bell_draw(streams_of[2], (D,), 1.0, 4.0, ((0, 4),), jnp.float32),
        "w_first": draw_w_first(jax.random.fold_in(streams_of[10], 71), 0),
        "b_first": jnp.clip(jax.random.uniform(streams_of[4], (FH,), jnp.float32, -3.140625, 3.140625), -3.140625, 3.140625),
        "freq": jnp.clip(jax.random.uniform(streams_of[5], (FH,), jnp.float32, 0.5, 2.0), 0.5, 2.0),
        "w_mid": draw_w_mid(jax.random.fold_in(streams_of[10], 71), 0),
        "w_last": bell_draw(streams_of[7], (FH, D), (FH * 256) ** -0.5, 0.046875, ((1, 4),), jnp.float32),
        "rate": jnp.clip(jnp.exp(math.log(0.08) - 6.302863 * jax.random.uniform(streams_of[8], (D,), jnp.float32) ** block_scale(streams_of[8], (D,), ((0, 4),), -0.2, 0.2)), 0.00014648438, 0.08),
        "out_w": bell_draw(streams_of[9], (D, D), D ** -0.5, 0.125, ((0, 4),)),
    }


def make_filter(w_first, b_first, freq, w_mid, w_last, rate, start, count):
    highest = lax.Precision.HIGHEST
    position = (start + jnp.arange(count)).astype(jnp.float32)
    bands = jnp.arange(1, BANDS + 1).astype(jnp.float32)
    angles = 2.0 * math.pi * position[:, None] * bands[None, :] / K
    features = jnp.concatenate([position[:, None] / K, jnp.cos(angles), jnp.sin(angles)], 1)
    first = jnp.sin(freq * (jnp.dot(features, w_first, precision=highest) + b_first))
    second = jnp.sin(freq * jnp.dot(first, w_mid, precision=highest))
    raw = jnp.dot(second, w_last, precision=highest)
    return (raw * jnp.exp(-rate[None, :] * position[:, None])).astype(jnp.bfloat16)


def reference(signal, gate, skip, w_first, b_first, freq, w_mid, w_last, rate, out_w):
    filt = make_filter(w_first, b_first, freq, w_mid, w_last, rate, 0, K)
    size_fft = 1 << (LENGTH + K - 2).bit_length()
    blocks = D // 128
    values = signal.astype(jnp.float32).reshape(LENGTH, blocks, 128).transpose(1, 0, 2)
    kernels = filt.astype(jnp.float32).reshape(K, blocks, 128).transpose(1, 0, 2)

    def convolve(pair):
        left, right = pair
        product = jnp.fft.rfft(left, n=size_fft, axis=0) * jnp.fft.rfft(right, n=size_fft, axis=0)
        return jnp.fft.irfft(product, n=size_fft, axis=0)[:LENGTH]

    conv = lax.map(convolve, (values, kernels)).transpose(1, 0, 2).reshape(LENGTH, D)
    mixed = (gate.astype(jnp.float32) * (conv + skip[None, :] * signal.astype(jnp.float32))).astype(jnp.bfloat16)
    return jnp.dot(mixed, out_w, preferred_element_type=jnp.float32).astype(jnp.bfloat16)
```

```python
import functools
import math

import jax
import jax.numpy as jnp
import numpy as np
from jax import lax
from jax.experimental import pallas as pl
from jax.experimental.pallas import tpu as pltpu
from jax.sharding import PartitionSpec as P

K = 2048
BANDS = 16
BLOCK = 128
VMEM = pltpu.MemorySpace.VMEM
SMEM = pltpu.MemorySpace.SMEM
BF16 = jnp.bfloat16
F32 = jnp.float32
HIGHEST = lax.Precision.HIGHEST


def feature_table():
    taps = np.arange(K, dtype=np.float64)
    bands = np.arange(1, BANDS + 1, dtype=np.float64)
    angles = 2.0 * np.pi * ((taps[None, :] * bands[:, None]) % K) / K
    return np.concatenate([taps[None, :] / K, np.cos(angles), np.sin(angles)], 0).astype(np.float32)


def split(table):
    table = np.asarray(table, np.float32)
    high = table.astype(BF16)
    low = (table - high.astype(np.float32)).astype(BF16)
    return high, low


def forward_table():
    size = 2 * BLOCK
    samples = np.arange(size)
    freqs = np.arange(BLOCK)
    phase = 2.0 * np.pi * ((samples[:, None] * freqs[None, :]) % size) / size
    real = np.cos(phase)
    imag = -np.sin(phase)
    imag[:, 0] = 1.0 - 2.0 * (samples % 2)
    return np.concatenate([real, imag], 1)


def backward_table():
    size = 2 * BLOCK
    samples = np.arange(BLOCK, size)
    freqs = np.arange(BLOCK)
    phase = 2.0 * np.pi * ((freqs[:, None] * samples[None, :]) % size) / size
    real = 2.0 * np.cos(phase)
    imag = -2.0 * np.sin(phase)
    real[0] = 1.0
    imag[0] = 1.0 - 2.0 * (samples % 2)
    return np.concatenate([real, imag], 0) / size


def dot(a, b):
    return jnp.dot(a, b, preferred_element_type=F32)


def sine(x):
    turns = jnp.round(x * (1.0 / math.pi))
    r = x - turns * 3.140625
    r = r - turns * 9.67502593994140625e-4
    r = r - turns * 1.50995799097e-7
    odd = turns - 2.0 * jnp.floor(turns * 0.5)
    sign = 1.0 - 2.0 * odd
    s = r * r
    p = -2.5052108385e-8
    p = p * s + 2.7557319224e-6
    p = p * s - 1.9841269841e-4
    p = p * s + 8.3333333333e-3
    p = p * s - 1.6666666667e-1
    return sign * (r + r * (s * p))


def filter_kernel(feat, w_first, bias, freq, w_mid, w_last, rate, table, real_out, imag_out, real2_out):
    first = sine(freq[...] * (jnp.dot(w_first[...], feat[...], precision=HIGHEST) + bias[...]))
    second = sine(freq[...] * jnp.dot(w_mid[...], first, precision=HIGHEST))
    raw = jnp.dot(w_last[...], second, precision=HIGHEST)
    channels, taps = raw.shape
    position = lax.broadcasted_iota(jnp.int32, (1, taps), 1).astype(F32)
    filt = (raw * jnp.exp(-rate[...] * position)).astype(BF16)
    count = taps // BLOCK
    rows = jnp.concatenate([filt[:, j * BLOCK : (j + 1) * BLOCK] for j in range(count)], 0)
    spec = dot(jnp.concatenate([rows, rows], 1), table[...])
    real, imag = spec[:, :BLOCK], spec[:, BLOCK:]
    lane = lax.broadcasted_iota(jnp.int32, real.shape, 1)
    shape = (count, channels, BLOCK)
    real_out[...] = real.reshape(shape)
    imag_out[...] = jnp.where(lane == 0, 0.0, imag).reshape(shape)
    real2_out[...] = jnp.where(lane == 0, imag, real).reshape(shape)


def conv_kernel(pieces, index, real, imag, real2, table_high, table_low, back_high, back_low, *refs):
    ins, outs = refs[:pieces], refs[pieces : 2 * pieces]
    samples, spec, total, result = refs[2 * pieces :]
    me = index[0]
    blocks, channels = total.shape[0], total.shape[1]
    per = ins[0].shape[2] // BLOCK
    samples[0] = jnp.zeros((channels, BLOCK), BF16)
    for k in range(pieces):
        for r in range(2):
            place = lax.bitwise_xor(me, 2 * k + r) * per
            for part in range(per):
                samples[place + (1 + part)] = ins[k][r, :, part * BLOCK : (part + 1) * BLOCK]
    before = samples[0:blocks].reshape(blocks * channels, BLOCK)
    current = samples[1 : blocks + 1].reshape(blocks * channels, BLOCK)
    window = jnp.concatenate([before, current], 1)
    spec[...] = (dot(window, table_high[...]) + dot(window, table_low[...])).reshape(spec.shape)
    taps = real.shape[0]

    def group(g, carry):
        at = pl.ds(pl.multiple_of(g * 8, 8), 8)
        for k in range(blocks):
            acc_real = acc_imag = None
            for j in range(min(k + 1, taps)):
                x_real = spec[k - j, at, :BLOCK]
                x_imag = spec[k - j, at, BLOCK:]
                f_real, f_imag, f_real2 = real[j, at, :], imag[j, at, :], real2[j, at, :]
                term_real = x_real * f_real - x_imag * f_imag
                term_imag = x_real * f_imag + x_imag * f_real2
                acc_real = term_real if acc_real is None else acc_real + term_real
                acc_imag = term_imag if acc_imag is None else acc_imag + term_imag
            total[k, at, :BLOCK] = acc_real
            total[k, at, BLOCK:] = acc_imag
        return carry

    lax.fori_loop(0, channels // 8, group, 0)
    sums = total[...].reshape(blocks * channels, 2 * BLOCK)
    high = sums.astype(BF16)
    low = (sums - high.astype(F32)).astype(BF16)
    conv = dot(high, back_high[...]) + dot(low, back_high[...]) + dot(high, back_low[...])
    result[...] = conv.astype(BF16).reshape(result.shape)
    for k in range(pieces):
        for r in range(2):
            place = lax.bitwise_xor(me, 2 * k + r) * per
            for part in range(per):
                outs[k][r, :, part * BLOCK : (part + 1) * BLOCK] = result[place + part]


def mix_kernel(pieces, index, signal, gate, skip, other, *refs):
    ins, (keep_out, send_out), conv = refs[:pieces], refs[pieces : pieces + 2], refs[pieces + 2]
    me, core = index[0], index[1]
    channels = ins[0].shape[1]
    for k in range(pieces):
        conv[lax.bitwise_xor(me, 2 * k)] = ins[k][0]
        conv[lax.bitwise_xor(me, 2 * k + 1)] = other[k]
    turned = conv[...].reshape(-1, conv.shape[-1]).T.astype(F32)
    mixed = (
        gate[...].astype(F32) * (turned + skip[...] * signal[...].astype(F32))
    ).astype(BF16)
    half = mixed.shape[0] // 2
    low, high = mixed[:half], mixed[half:]
    keep_out[...] = jnp.where(core == 0, low, high)
    send_out[...] = jnp.where(core == 0, high, low)


def terms_kernel(head_xors, index, mine, theirs, own_w, other_w, *outs):
    head = index[2]
    width = outs[0].shape[1]
    for flip, out in zip(head_xors, outs):
        at = pl.ds(pl.multiple_of(lax.bitwise_xor(head, flip) * width, width), width)
        out[...] = (dot(mine[...], own_w[:, at]) + dot(theirs[...], other_w[:, at])).astype(out.dtype)


def sum_kernel(index, own, a, b, c, out):
    core = index[1]
    half = own.shape[0]
    here = own[...] + a[...].astype(F32)
    there = c[...].astype(F32) + b[...].astype(F32)
    out[pl.ds(pl.multiple_of(core * half, half), half), :] = here.astype(BF16)
    out[pl.ds(pl.multiple_of((1 - core) * half, half), half), :] = there.astype(BF16)


def turn_kernel(x, out):
    out[...] = x[...].T


def spec_of(space):
    return pl.BlockSpec(memory_space=space)


def call(kernel, outs, *args, scratch=(), flops=0, name=None, scalars=0):
    return pl.pallas_call(
        kernel,
        out_shape=outs,
        in_specs=[spec_of(SMEM)] * scalars + [spec_of(VMEM)] * (len(args) - scalars),
        out_specs=jax.tree.map(lambda _: spec_of(VMEM), outs),
        scratch_shapes=list(scratch),
        cost_estimate=pl.CostEstimate(flops=flops, bytes_accessed=0, transcendentals=0),
        name=name,
    )(*args)


def shape(dims, dtype=BF16):
    return jax.ShapeDtypeStruct(dims, dtype)


def flip(x, axis, by):
    size = lax.axis_size(axis)
    return lax.ppermute(x, axis, [(i, i ^ by) for i in range(size)])


def spread(signal, gate, skip, w_first, b_first, freq, w_mid, w_last, rate, out_w):
    length_local, channels = signal.shape
    ranks = lax.axis_size("seq")
    pieces = ranks // 2
    share = channels // ranks
    blocks = ranks * length_local // BLOCK
    taps = K // BLOCK
    me = lax.axis_index("seq")
    head = lax.axis_index("head")
    side = me % 2
    index = jnp.stack([me, head % 2, head]).astype(jnp.int32)
    other_w = flip(out_w, "head", 1)

    turned = call(turn_kernel, shape((channels, length_local)), signal, name="turn")
    turned = turned.reshape(pieces, 2, share, length_local)
    keep = lax.dynamic_index_in_dim(turned, side, 1, keepdims=True)
    send = lax.dynamic_index_in_dim(turned, 1 - side, 1, keepdims=True)
    stack = jnp.concatenate([keep, flip(send, "seq", 1)], 1)
    parts = [
        lax.dynamic_index_in_dim(stack, (me // 2) ^ k, 0, keepdims=False) for k in range(pieces)
    ]
    parts = [flip(part, "seq", 2 * k) if k else part for k, part in enumerate(parts)]

    column = lambda v: v.reshape(-1, 1)
    forward_high, forward_low = split(forward_table())
    back_high, back_low = split(backward_table())
    filter_table = np.concatenate([forward_high[:BLOCK], forward_low[:BLOCK]], 0)
    spectrum = shape((taps, share, BLOCK), F32)
    real, imag, real2 = call(
        filter_kernel,
        (spectrum,) * 3,
        feature_table(),
        w_first.T,
        column(b_first),
        column(freq),
        w_mid.T,
        lax.dynamic_slice_in_dim(w_last, me * share, share, 1).T,
        column(lax.dynamic_slice_in_dim(rate, me * share, share, 0)),
        filter_table,
        flops=2_000_000_000,
        name="filter",
    )

    piece = shape((2, share, length_local))
    convs = call(
        functools.partial(conv_kernel, pieces),
        (piece,) * pieces,
        index,
        real,
        imag,
        real2,
        forward_high,
        forward_low,
        back_high,
        back_low,
        *parts,
        scratch=[
            pltpu.VMEM((blocks + 1, share, BLOCK), BF16),
            pltpu.VMEM((blocks, share, 2 * BLOCK), F32),
            pltpu.VMEM((blocks, share, 2 * BLOCK), F32),
            pltpu.VMEM((blocks, share, BLOCK), BF16),
        ],
        flops=2_000_000_000,
        name="conv",
        scalars=1,
    )

    convs = [flip(conv, "seq", 2 * k) if k else conv for k, conv in enumerate(convs)]
    other = flip(jnp.stack([conv[1] for conv in convs]), "seq", 1)
    half = length_local // 2
    keep, send = call(
        functools.partial(mix_kernel, pieces),
        (shape((half, channels)),) * 2,
        index,
        signal,
        gate,
        skip.reshape(1, -1),
        other,
        *convs,
        scratch=[pltpu.VMEM((ranks, share, length_local), BF16)],
        flops=500_000_000,
        name="mix",
        scalars=1,
    )
    got = flip(send, "head", 1)
    width = out_w.shape[1] // lax.axis_size("head")
    terms = shape((half, width))
    a, b = call(
        functools.partial(terms_kernel, (2, 3)),
        (terms, terms),
        index,
        keep,
        got,
        out_w,
        other_w,
        flops=500_000_000,
        name="terms_far",
        scalars=1,
    )
    a, b = flip(a, "head", 2), flip(b, "head", 3)
    c, own = call(
        functools.partial(terms_kernel, (1, 0)),
        (terms, shape((half, width), F32)),
        index,
        keep,
        got,
        out_w,
        other_w,
        flops=500_000_000,
        name="terms_near",
        scalars=1,
    )
    c = flip(c, "head", 1)
    return call(sum_kernel, shape((length_local, width)), index, own, a, b, c, name="sum", scalars=1)


def shifted(x, axis, by):
    size = lax.axis_size(axis)
    pairs = [(i, i + by) for i in range(size) if 0 <= i + by < size]
    return lax.ppermute(x, axis, pairs)


def make_filter(w_first, b_first, freq, w_mid, w_last, rate, count):
    position = jnp.arange(count).astype(jnp.float32)
    bands = jnp.arange(1, BANDS + 1).astype(jnp.float32)
    angles = 2.0 * math.pi * position[:, None] * bands[None, :] / K
    features = jnp.concatenate([position[:, None] / K, jnp.cos(angles), jnp.sin(angles)], 1)
    first = jnp.sin(freq * (jnp.dot(features, w_first, precision=HIGHEST) + b_first))
    second = jnp.sin(freq * jnp.dot(first, w_mid, precision=HIGHEST))
    raw = jnp.dot(second, w_last, precision=HIGHEST)
    return (raw * jnp.exp(-rate[None, :] * position[:, None])).astype(jnp.bfloat16)


def transform_tables(block):
    doubled = 2 * block
    taps = jnp.arange(block)
    freqs = jnp.arange(block)
    outputs = jnp.arange(doubled)
    scale_angle = 2.0 * math.pi / doubled
    phase = (freqs[:, None] * taps[None, :] % doubled).astype(jnp.float32) * scale_angle
    alternate = (1 - 2 * (taps % 2)).astype(jnp.float32)
    forward_real = jnp.cos(phase)
    forward_imag = jnp.where(freqs[:, None] == 0, alternate[None, :], -jnp.sin(phase))
    phase_back = (outputs[:, None] * freqs[None, :] % doubled).astype(jnp.float32) * scale_angle
    alternate_back = (1 - 2 * (outputs % 2)).astype(jnp.float32)
    weights = jnp.where(freqs == 0, 1.0, 2.0).astype(jnp.float32)
    back_real = weights[None, :] * jnp.cos(phase_back) / doubled
    back_imag = (
        jnp.where(freqs[None, :] == 0, alternate_back[:, None], -2.0 * jnp.sin(phase_back))
        / doubled
    )
    return (forward_real, forward_imag, back_real, back_imag)


def long_convolve(padded, filt, length_local):
    channels = padded.shape[1]
    block = min(128, length_local)
    segments = K // block
    out_blocks = length_local // block
    in_blocks = padded.shape[0] // block
    forward_real, forward_imag, back_real, back_imag = transform_tables(block)
    values = padded.astype(jnp.float32).reshape(in_blocks, block, channels)
    kernels = filt.astype(jnp.float32).reshape(segments, block, channels)[::-1]
    spec_real = jnp.einsum("ft,ntc->nfc", forward_real, values, precision=HIGHEST)
    spec_imag = jnp.einsum("ft,ntc->nfc", forward_imag, values, precision=HIGHEST)
    kern_real = jnp.einsum("ft,ntc->nfc", forward_real, kernels, precision=HIGHEST)
    kern_imag = jnp.einsum("ft,ntc->nfc", forward_imag, kernels, precision=HIGHEST)
    upper = (jnp.arange(block) >= 1).astype(jnp.float32)[:, None]
    sums_real = []
    sums_imag = []
    for index in range(out_blocks + 1):
        window_real = spec_real[index : index + segments]
        window_imag = spec_imag[index : index + segments]
        both_imag = kern_imag * window_imag
        sums_real.append(jnp.sum(kern_real * window_real - upper * both_imag, 0))
        cross = kern_real * window_imag + kern_imag * window_real
        sums_imag.append(jnp.sum(upper * cross + (1.0 - upper) * both_imag, 0))
    total_real = jnp.stack(sums_real, 0)
    total_imag = jnp.stack(sums_imag, 0)
    pieces = jnp.einsum("tf,kfc->ktc", back_real, total_real, precision=HIGHEST)
    pieces = pieces + jnp.einsum("tf,kfc->ktc", back_imag, total_imag, precision=HIGHEST)
    joined = pieces[1:, :block] + pieces[:-1, block:]
    return joined.reshape(length_local, channels)


def halo(signal, gate, skip, w_first, b_first, freq, w_mid, w_last, rate, out_w):
    length_local, channels = signal.shape
    filt = make_filter(w_first, b_first, freq, w_mid, w_last, rate, K)
    reach = K // length_local
    earlier = [shifted(signal, "seq", step) for step in range(reach, 0, -1)]
    padded = jnp.concatenate(earlier + [signal], 0)
    conv = long_convolve(padded, filt, length_local)
    mixed = (gate.astype(jnp.float32) * (conv + skip[None, :] * signal.astype(jnp.float32))).astype(
        jnp.bfloat16
    )
    terms = jnp.dot(mixed, out_w, preferred_element_type=jnp.float32)
    result = lax.psum_scatter(terms, "head", scatter_dimension=1, tiled=True)
    return result.astype(jnp.bfloat16)


def local(signal, *rest):
    ranks, heads = lax.axis_size("seq"), lax.axis_size("head")
    length_local, channels = signal.shape
    small = ranks * length_local <= K and heads == 4
    fits = ranks >= 2 and ranks & (ranks - 1) == 0 and channels % (16 * ranks) == 0
    if small and fits and length_local % (2 * BLOCK) == 0:
        return spread(signal, *rest)
    return halo(signal, *rest)


def solution(mesh):
    placed = (
        P("seq", "head"),
        P("seq", "head"),
        P("head"),
        P(),
        P(),
        P(),
        P(),
        P(None, "head"),
        P("head"),
        P("head", None),
    )
    return jax.shard_map(
        local, mesh=mesh, in_specs=placed, out_specs=P("seq", "head"), check_vma=False
    )
```

```python
import functools
import math

import jax
import jax.numpy as jnp
import numpy as np
from jax import lax
from jax.experimental import pallas as pl
from jax.experimental.pallas import tpu as pltpu
from jax.sharding import PartitionSpec as P


K = 2048
BANDS = 16
BLOCK = 128
VMEM = pltpu.MemorySpace.VMEM
BF16 = jnp.bfloat16
F32 = jnp.float32
HIGHEST = lax.Precision.HIGHEST


def feature_table():
    taps = np.arange(K, dtype=np.float64)
    bands = np.arange(1, BANDS + 1, dtype=np.float64)
    angles = 2.0 * np.pi * ((taps[None, :] * bands[:, None]) % K) / K
    return np.concatenate([taps[None, :] / K, np.cos(angles), np.sin(angles)], 0).astype(np.float32)


def split(table):
    table = np.asarray(table, np.float32)
    high = table.astype(BF16)
    low = (table - high.astype(np.float32)).astype(BF16)
    return high, low


def forward_table():
    size = 2 * BLOCK
    samples = np.arange(size)
    freqs = np.arange(BLOCK)
    phase = 2.0 * np.pi * ((samples[:, None] * freqs[None, :]) % size) / size
    real = np.cos(phase)
    imag = -np.sin(phase)
    imag[:, 0] = 1.0 - 2.0 * (samples % 2)
    return np.concatenate([real, imag], 1)


def backward_table():
    size = 2 * BLOCK
    samples = np.arange(BLOCK, size)
    freqs = np.arange(BLOCK)
    phase = 2.0 * np.pi * ((freqs[:, None] * samples[None, :]) % size) / size
    real = 2.0 * np.cos(phase)
    imag = -2.0 * np.sin(phase)
    real[0] = 1.0
    imag[0] = 1.0 - 2.0 * (samples % 2)
    return np.concatenate([real, imag], 0) / size


def dot(a, b):
    return jnp.dot(a, b, preferred_element_type=F32)


def sine(x):
    turns = jnp.round(x * (1.0 / math.pi))
    r = x - turns * 3.140625
    r = r - turns * 9.67502593994140625e-4
    r = r - turns * 1.50995799097e-7
    odd = turns - 2.0 * jnp.floor(turns * 0.5)
    sign = 1.0 - 2.0 * odd
    s = r * r
    p = -2.5052108385e-8
    p = p * s + 2.7557319224e-6
    p = p * s - 1.9841269841e-4
    p = p * s + 8.3333333333e-3
    p = p * s - 1.6666666667e-1
    return sign * (r + r * (s * p))


def column(row):
    n = row.shape[1]
    square = (n, n)
    diagonal = lax.broadcasted_iota(jnp.int32, square, 0) == lax.broadcasted_iota(jnp.int32, square, 1)
    return jnp.sum(jnp.where(diagonal, jnp.broadcast_to(row, square), 0.0), 1, keepdims=True)


def dot_first(a, b):
    return lax.dot_general(
        a, b, (((0,), (0,)), ((), ())), precision=HIGHEST, preferred_element_type=F32
    )


def share_of(share):
    me = lax.axis_index("seq")
    groups = 128 // share
    lanes = pl.ds(pl.multiple_of((me // groups) * 128, 128), 128)
    rows = pl.ds(pl.multiple_of(lax.rem(me, groups) * share, share), share)
    return lanes, rows


def fetch(sources, targets, sems):
    copies = [
        pltpu.make_async_copy(source, target, sems.at[n])
        for n, (source, target) in enumerate(zip(sources, targets))
    ]
    for copy in copies:
        copy.start()
    return copies


def filter_kernel(count, *refs):
    out, weights, scales, sems = refs[count], refs[2 * count + 1], refs[2 * count + 2], refs[2 * count + 3]
    held = refs[count + 1 : 2 * count + 1]
    for copy in fetch(refs[:count], held, sems):
        copy.wait()
    feat, w_first, bias, freq, w_mid, w_last, rate, table = held
    share = out.shape[1]
    lanes, own = share_of(share)
    freqs = column(freq[...])
    first = sine(freqs * (dot_first(w_first[...], feat[...]) + column(bias[...])))
    second = sine(freqs * dot_first(w_mid[...], first))
    weights[...] = w_last[:, lanes].T
    scales[...] = jnp.broadcast_to(column(rate[:, lanes]), scales.shape)
    raw = jnp.dot(weights[own, :], second, precision=HIGHEST)
    taps = raw.shape[1]
    decay = scales[own, :][:, :1]
    position = lax.broadcasted_iota(jnp.int32, (1, taps), 1).astype(F32)
    filt = (raw * jnp.exp(-decay * position)).astype(BF16)
    count = taps // BLOCK
    rows = jnp.concatenate([filt[:, j * BLOCK : (j + 1) * BLOCK] for j in range(count)], 0)
    spec = dot(jnp.concatenate([rows, rows], 1), table[...])
    out[...] = spec.reshape(out.shape)


def conv_kernel(pieces, filt, table_high, table_low, back_high, back_low, *refs):
    own_in, beside_in = refs[:2]
    ins, outs = refs[2 : pieces + 1], refs[pieces + 1 : 2 * pieces + 2]
    samples, spec, total, result = refs[2 * pieces + 2 :]
    me = lax.axis_index("seq")
    blocks, channels = total.shape[0], total.shape[1]
    per = own_in.shape[1] // BLOCK
    samples[0] = jnp.zeros((channels, BLOCK), BF16)

    def place(values, flips):
        at = lax.bitwise_xor(me, flips) * per
        for part in range(per):
            samples[at + (1 + part)] = values[:, part * BLOCK : (part + 1) * BLOCK]

    place(own_in[...], 0)
    place(beside_in[0], 1)
    for k in range(1, pieces):
        for side in range(2):
            place(ins[k - 1][side], 2 * k + side)
    before = samples[0:blocks].reshape(blocks * channels, BLOCK)
    current = samples[1 : blocks + 1].reshape(blocks * channels, BLOCK)
    window = jnp.concatenate([before, current], 1)
    spec[...] = (dot(window, table_high[...]) + dot(window, table_low[...])).reshape(spec.shape)
    taps = filt.shape[0]

    packed = lax.broadcasted_iota(jnp.int32, (8, BLOCK), 1) == 0

    def group(g, carry):
        at = pl.ds(pl.multiple_of(g * 8, 8), 8)
        for k in range(blocks):
            both_real = both_imag = cross = None
            for j in range(min(k + 1, taps)):
                x_real, x_imag = spec[k - j, at, :BLOCK], spec[k - j, at, BLOCK:]
                f_real, f_imag = filt[j, at, :BLOCK], filt[j, at, BLOCK:]
                terms = (x_real * f_real, x_imag * f_imag, x_real * f_imag + x_imag * f_real)
                if j == 0:
                    both_real, both_imag, cross = terms
                else:
                    both_real, both_imag, cross = both_real + terms[0], both_imag + terms[1], cross + terms[2]
            total[k, at, :BLOCK] = both_real - jnp.where(packed, 0.0, both_imag)
            total[k, at, BLOCK:] = jnp.where(packed, both_imag, cross)
        return carry

    lax.fori_loop(0, channels // 8, group, 0)
    sums = total[...].reshape(blocks * channels, 2 * BLOCK)
    high = sums.astype(BF16)
    low = (sums - high.astype(F32)).astype(BF16)
    conv = dot(high, back_high[...]) + dot(low, back_high[...]) + dot(high, back_low[...])
    result[...] = conv.astype(BF16).reshape(result.shape)

    def taken(flips):
        at = lax.bitwise_xor(me, flips) * per
        return jnp.concatenate([result[at + part] for part in range(per)], 1)

    outs[0][...] = taken(0)
    outs[1][...] = taken(1)
    for k in range(1, pieces):
        for side in range(2):
            outs[k + 1][side] = taken(2 * k + side)


def mix_kernel(pieces, signal, gate, skip, own_in, *refs):
    ins, beside = refs[: pieces - 1], refs[pieces - 1 : pieces - 1 + pieces // 2]
    keep_out, send_out, conv = refs[-3:]
    me = lax.axis_index("seq")
    core = lax.rem(lax.axis_index("head"), 2)
    conv[me] = own_in[...]
    for k in range(1, pieces):
        conv[lax.bitwise_xor(me, 2 * k)] = ins[k - 1][0]
    for k in range(pieces):
        conv[lax.bitwise_xor(me, 2 * k + 1)] = beside[k // 2][k % 2]
    turned = conv[...].reshape(-1, conv.shape[-1]).T.astype(F32)
    mixed = (gate[...].astype(F32) * (turned + skip[...] * signal[...].astype(F32))).astype(BF16)
    half = keep_out.shape[0]
    low, high = mixed[:half], mixed[half:]
    keep_out[...] = jnp.where(core == 0, low, high)
    send_out[...] = jnp.where(core == 0, high, low)


def project_kernel(flips, own, other, own_w, other_w, *outs):
    head = lax.axis_index("head")
    width = outs[0].shape[1]
    for flip, out in zip(flips, outs):
        columns = pl.ds(pl.multiple_of(lax.bitwise_xor(head, flip) * width, width), width)
        terms = dot(own[...], own_w[:, columns]) + dot(other[...], other_w[:, columns])
        out[...] = terms.astype(out.dtype)


def sum_kernel(own, a, b, c, out):
    core = lax.rem(lax.axis_index("head"), 2)
    half = own.shape[0]
    here = own[...] + a[...].astype(F32)
    there = c[...].astype(F32) + b[...].astype(F32)
    out[pl.ds(pl.multiple_of(core * half, half), half), :] = here.astype(BF16)
    out[pl.ds(pl.multiple_of((1 - core) * half, half), half), :] = there.astype(BF16)


def turn_kernel(pieces, signal, *refs):
    own, beside = refs[:pieces], refs[pieces : pieces + pieces // 2]
    held, turned, sems = refs[pieces + pieces // 2 :]
    me = lax.axis_index("seq")
    share = own[0].shape[0]
    parts = held.shape[0]
    wide = held.shape[2]
    sources = [signal.at[:, n * wide : (n + 1) * wide] for n in range(parts)]
    copies = fetch(sources, [held.at[n] for n in range(parts)], sems)
    for n, copy in enumerate(copies):
        copy.wait()
        turned[n * (wide // share) : (n + 1) * (wide // share)] = held[n].T.reshape(-1, share, held.shape[1])
    for k in range(pieces):
        own[k][...] = turned[lax.bitwise_xor(me, 2 * k)]
        beside[k // 2][k % 2] = turned[lax.bitwise_xor(me, 2 * k + 1)]


def call(kernel, outs, *args, scratch=(), flops=0, grant=12, space=VMEM):
    run = pl.pallas_call(
        kernel,
        out_shape=outs,
        in_specs=[pl.BlockSpec(memory_space=space)] * len(args),
        out_specs=jax.tree.map(lambda _: pl.BlockSpec(memory_space=VMEM), outs),
        scratch_shapes=list(scratch),
        cost_estimate=pl.CostEstimate(flops=flops, bytes_accessed=0, transcendentals=0),
        compiler_params=pltpu.CompilerParams(vmem_limit_bytes=grant << 20),
    )
    if space is not VMEM:
        args = [pltpu.with_memory_space_constraint(arg, space) for arg in args]
    return run(*args)


def shape(dims, dtype=BF16):
    return jax.ShapeDtypeStruct(dims, dtype)


def flip(x, axis, by):
    size = lax.axis_size(axis)
    return lax.ppermute(x, axis, [(i, i ^ by) for i in range(size)])


def spread(signal, gate, skip, w_first, b_first, freq, w_mid, w_last, rate, out_w):
    length_local, channels = signal.shape
    ranks, heads = lax.axis_size("seq"), lax.axis_size("head")
    pieces = ranks // 2
    share = channels // ranks
    blocks = ranks * length_local // BLOCK
    taps = K // BLOCK
    half = length_local // 2
    width = out_w.shape[1] // heads
    row = lambda v: v.reshape(1, -1)

    piece, pair = shape((share, length_local)), shape((2, share, length_local))
    *own, near, far = call(
        functools.partial(turn_kernel, pieces),
        (piece,) * pieces + (pair,) * 2,
        signal,
        scratch=[
            pltpu.VMEM((channels // 128, length_local, 128), BF16),
            pltpu.VMEM((ranks, share, length_local), BF16),
            pltpu.SemaphoreType.DMA((channels // 128,)),
        ],
        space=pltpu.HBM,
    )
    far = flip(far, "seq", 1)
    near = flip(near, "seq", 1)
    beside = [near[0], near[1], far[0], far[1]]
    parts = {k: flip(jnp.stack([own[k], beside[k]]), "seq", 2 * k) for k in (2, 3, 1)}

    forward_high, forward_low = split(forward_table())
    back_high, back_low = split(backward_table())
    filter_table = np.concatenate([forward_high[:BLOCK], forward_low[:BLOCK]], 0)
    operands = (
        jnp.asarray(feature_table()),
        w_first,
        row(b_first),
        row(freq),
        w_mid,
        w_last,
        row(rate),
        jnp.asarray(filter_table),
    )
    filt = call(
        functools.partial(filter_kernel, len(operands)),
        shape((taps, share, 2 * BLOCK), F32),
        *operands,
        scratch=[pltpu.VMEM(v.shape, v.dtype) for v in operands]
        + [
            pltpu.VMEM((128, w_last.shape[0]), F32),
            pltpu.VMEM((128, BLOCK), F32),
            pltpu.SemaphoreType.DMA((len(operands),)),
        ],
        flops=5_000_000_000,
        space=pltpu.HBM,
    )
    other_w = flip(out_w, "head", 1)
    conv_own, conv_beside, *convs = call(
        functools.partial(conv_kernel, pieces),
        (piece,) * 2 + (pair,) * (pieces - 1),
        filt,
        forward_high,
        forward_low,
        back_high,
        back_low,
        own[0],
        near,
        *[parts[k] for k in range(1, pieces)],
        scratch=[
            pltpu.VMEM((blocks + 1, share, BLOCK), BF16),
            pltpu.VMEM((blocks, share, 2 * BLOCK), F32),
            pltpu.VMEM((blocks, share, 2 * BLOCK), F32),
            pltpu.VMEM((blocks, share, BLOCK), BF16),
        ],
        flops=3_000_000_000,
    )

    got = {k: flip(convs[k - 1], "seq", 2 * k) for k in (2, 3, 1)}
    near = flip(jnp.stack([conv_beside, got[1][1]]), "seq", 1)
    far = flip(jnp.stack([got[2][1], got[3][1]]), "seq", 1)
    mixed = shape((half, channels))
    keep, send = call(
        functools.partial(mix_kernel, pieces),
        (mixed, mixed),
        signal,
        gate,
        row(skip),
        conv_own,
        got[1],
        got[2],
        got[3],
        near,
        far,
        scratch=[pltpu.VMEM((ranks, share, length_local), BF16)],
        flops=500_000_000,
    )
    received = flip(send, "head", 1)
    terms, wide = shape((half, width)), shape((half, width), F32)
    a, b, c, here = call(
        functools.partial(project_kernel, (2, 3, 1, 0)),
        (terms, terms, wide, wide),
        keep,
        received,
        out_w,
        other_w,
        flops=500_000_000,
    )
    a, b, c = flip(a, "head", 2), flip(b, "head", 3), flip(c, "head", 1)
    return call(sum_kernel, shape((length_local, width)), here, a, b, c)


def shifted(x, axis, by):
    size = lax.axis_size(axis)
    pairs = [(i, i + by) for i in range(size) if 0 <= i + by < size]
    return lax.ppermute(x, axis, pairs)


def make_filter(w_first, b_first, freq, w_mid, w_last, rate, count):
    position = jnp.arange(count).astype(jnp.float32)
    bands = jnp.arange(1, BANDS + 1).astype(jnp.float32)
    angles = 2.0 * math.pi * position[:, None] * bands[None, :] / K
    features = jnp.concatenate([position[:, None] / K, jnp.cos(angles), jnp.sin(angles)], 1)
    first = jnp.sin(freq * (jnp.dot(features, w_first, precision=HIGHEST) + b_first))
    second = jnp.sin(freq * jnp.dot(first, w_mid, precision=HIGHEST))
    raw = jnp.dot(second, w_last, precision=HIGHEST)
    return (raw * jnp.exp(-rate[None, :] * position[:, None])).astype(jnp.bfloat16)


def transform_tables(block):
    doubled = 2 * block
    taps = jnp.arange(block)
    freqs = jnp.arange(block)
    outputs = jnp.arange(doubled)
    scale_angle = 2.0 * math.pi / doubled
    phase = (freqs[:, None] * taps[None, :] % doubled).astype(jnp.float32) * scale_angle
    alternate = (1 - 2 * (taps % 2)).astype(jnp.float32)
    forward_real = jnp.cos(phase)
    forward_imag = jnp.where(freqs[:, None] == 0, alternate[None, :], -jnp.sin(phase))
    phase_back = (outputs[:, None] * freqs[None, :] % doubled).astype(jnp.float32) * scale_angle
    alternate_back = (1 - 2 * (outputs % 2)).astype(jnp.float32)
    weights = jnp.where(freqs == 0, 1.0, 2.0).astype(jnp.float32)
    back_real = weights[None, :] * jnp.cos(phase_back) / doubled
    back_imag = (
        jnp.where(freqs[None, :] == 0, alternate_back[:, None], -2.0 * jnp.sin(phase_back))
        / doubled
    )
    return (forward_real, forward_imag, back_real, back_imag)


def long_convolve(padded, filt, length_local):
    channels = padded.shape[1]
    block = min(128, length_local)
    segments = K // block
    out_blocks = length_local // block
    in_blocks = padded.shape[0] // block
    forward_real, forward_imag, back_real, back_imag = transform_tables(block)
    values = padded.astype(jnp.float32).reshape(in_blocks, block, channels)
    kernels = filt.astype(jnp.float32).reshape(segments, block, channels)[::-1]
    spec_real = jnp.einsum("ft,ntc->nfc", forward_real, values, precision=HIGHEST)
    spec_imag = jnp.einsum("ft,ntc->nfc", forward_imag, values, precision=HIGHEST)
    kern_real = jnp.einsum("ft,ntc->nfc", forward_real, kernels, precision=HIGHEST)
    kern_imag = jnp.einsum("ft,ntc->nfc", forward_imag, kernels, precision=HIGHEST)
    upper = (jnp.arange(block) >= 1).astype(jnp.float32)[:, None]
    sums_real = []
    sums_imag = []
    for index in range(out_blocks + 1):
        window_real = spec_real[index : index + segments]
        window_imag = spec_imag[index : index + segments]
        both_imag = kern_imag * window_imag
        sums_real.append(jnp.sum(kern_real * window_real - upper * both_imag, 0))
        cross = kern_real * window_imag + kern_imag * window_real
        sums_imag.append(jnp.sum(upper * cross + (1.0 - upper) * both_imag, 0))
    total_real = jnp.stack(sums_real, 0)
    total_imag = jnp.stack(sums_imag, 0)
    pieces = jnp.einsum("tf,kfc->ktc", back_real, total_real, precision=HIGHEST)
    pieces = pieces + jnp.einsum("tf,kfc->ktc", back_imag, total_imag, precision=HIGHEST)
    joined = pieces[1:, :block] + pieces[:-1, block:]
    return joined.reshape(length_local, channels)


def halo(signal, gate, skip, w_first, b_first, freq, w_mid, w_last, rate, out_w):
    length_local, _ = signal.shape
    filt = make_filter(w_first, b_first, freq, w_mid, w_last, rate, K)
    reach = K // length_local
    earlier = [shifted(signal, "seq", step) for step in range(reach, 0, -1)]
    padded = jnp.concatenate(earlier + [signal], 0)
    conv = long_convolve(padded, filt, length_local)
    mixed = (gate.astype(jnp.float32) * (conv + skip[None, :] * signal.astype(jnp.float32))).astype(
        jnp.bfloat16
    )
    terms = jnp.dot(mixed, out_w, preferred_element_type=jnp.float32)
    result = lax.psum_scatter(terms, "head", scatter_dimension=1, tiled=True)
    return result.astype(jnp.bfloat16)


def local(signal, *rest):
    ranks, heads = lax.axis_size("seq"), lax.axis_size("head")
    length_local, channels = signal.shape
    share = channels // ranks
    small = ranks == 8 and ranks * length_local <= K and heads == 4 and length_local == 2 * BLOCK
    if small and channels % ranks == 0 and share % 16 == 0 and 128 % share == 0:
        return spread(signal, *rest)
    return halo(signal, *rest)


def solution(mesh):
    placed = (
        P("seq", "head"),
        P("seq", "head"),
        P("head"),
        P(),
        P(),
        P(),
        P(),
        P(None, "head"),
        P("head"),
        P("head", None),
    )
    return jax.shard_map(
        local, mesh=mesh, in_specs=placed, out_specs=P("seq", "head"), check_vma=False
    )
```

```python
import functools
import math

import jax
import jax.numpy as jnp
import numpy as np
from jax import lax
from jax.experimental import pallas as pl
from jax.experimental.pallas import tpu as pltpu
from jax.sharding import PartitionSpec as P


K = 2048
BANDS = 16
BLOCK = 128
VMEM = pltpu.MemorySpace.VMEM
BF16 = jnp.bfloat16
F32 = jnp.float32
HIGHEST = lax.Precision.HIGHEST


def feature_table():
    taps = np.arange(K, dtype=np.float64)
    bands = np.arange(1, BANDS + 1, dtype=np.float64)
    angles = 2.0 * np.pi * ((taps[None, :] * bands[:, None]) % K) / K
    return np.concatenate([taps[None, :] / K, np.cos(angles), np.sin(angles)], 0).astype(np.float32)


def split(table):
    table = np.asarray(table, np.float32)
    high = table.astype(BF16)
    low = (table - high.astype(np.float32)).astype(BF16)
    return high, low


def forward_table():
    size = 2 * BLOCK
    samples = np.arange(size)
    freqs = np.arange(BLOCK)
    phase = 2.0 * np.pi * ((samples[:, None] * freqs[None, :]) % size) / size
    real = np.cos(phase)
    imag = -np.sin(phase)
    imag[:, 0] = 1.0 - 2.0 * (samples % 2)
    return np.concatenate([real, imag], 1)


def backward_table():
    size = 2 * BLOCK
    samples = np.arange(BLOCK, size)
    freqs = np.arange(BLOCK)
    phase = 2.0 * np.pi * ((freqs[:, None] * samples[None, :]) % size) / size
    real = 2.0 * np.cos(phase)
    imag = -2.0 * np.sin(phase)
    real[0] = 1.0
    imag[0] = 1.0 - 2.0 * (samples % 2)
    return np.concatenate([real, imag], 0) / size


def dot(a, b):
    return jnp.dot(a, b, preferred_element_type=F32)


def sine(x):
    turns = jnp.round(x * (1.0 / math.pi))
    r = x - turns * 3.140625
    r = r - turns * 9.67502593994140625e-4
    r = r - turns * 1.50995799097e-7
    odd = turns - 2.0 * jnp.floor(turns * 0.5)
    sign = 1.0 - 2.0 * odd
    s = r * r
    p = -2.5052108385e-8
    p = p * s + 2.7557319224e-6
    p = p * s - 1.9841269841e-4
    p = p * s + 8.3333333333e-3
    p = p * s - 1.6666666667e-1
    return sign * (r + r * (s * p))


def column(row):
    n = row.shape[1]
    square = (n, n)
    diagonal = lax.broadcasted_iota(jnp.int32, square, 0) == lax.broadcasted_iota(jnp.int32, square, 1)
    return jnp.sum(jnp.where(diagonal, jnp.broadcast_to(row, square), 0.0), 1, keepdims=True)


def dot_first(a, b):
    return lax.dot_general(
        a, b, (((0,), (0,)), ((), ())), precision=HIGHEST, preferred_element_type=F32
    )


def fetch(sources, targets, sems):
    copies = [
        pltpu.make_async_copy(source, target, sems.at[n])
        for n, (source, target) in enumerate(zip(sources, targets))
    ]
    for copy in copies:
        copy.start()
    return copies


def hidden_kernel(count, *refs):
    out, held, sems = refs[count], refs[count + 1 : 2 * count + 1], refs[2 * count + 1]
    for copy in fetch(refs[:count], held, sems):
        copy.wait()
    feat, w_first, bias, freq, w_mid = held
    freqs = column(freq[...])
    first = sine(freqs * (dot_first(w_first[...], feat[...]) + column(bias[...])))
    out[...] = sine(freqs * dot_first(w_mid[...], first))


def filter_kernel(count, hidden, *refs):
    out, held, sems = refs[count], refs[count + 1 : 2 * count + 1], refs[2 * count + 1]
    for copy in fetch(refs[:count], held, sems):
        copy.wait()
    w_last, rate, table = held
    share = out.shape[1]
    own = pl.ds(pl.multiple_of((lax.axis_index("seq") // 2) * share, share), share)
    raw = dot_first(w_last[:, own], hidden[...])
    taps = raw.shape[1]
    position = lax.broadcasted_iota(jnp.int32, (1, taps), 1).astype(F32)
    filt = (raw * jnp.exp(-column(rate[:, own]) * position)).astype(BF16)
    blocks = taps // BLOCK
    rows = jnp.concatenate([filt[:, j * BLOCK : (j + 1) * BLOCK] for j in range(blocks)], 0)
    spec = dot(jnp.concatenate([rows, rows], 1), table[...])
    out[...] = spec.reshape(out.shape)


def conv_kernel(pieces, filt, table_high, table_low, back_high, back_low, *refs):
    ins, outs = refs[: 2 * pieces], refs[2 * pieces : 3 * pieces]
    samples, spec, total, result = refs[3 * pieces :]
    me = lax.axis_index("seq")
    side = lax.rem(me, 2)
    blocks, channels = samples.shape[0] - 1, samples.shape[1]
    per = ins[0].shape[1] // BLOCK
    samples[0] = jnp.zeros((channels, BLOCK), BF16)
    for flips, piece in enumerate(ins):
        at = lax.bitwise_xor(me, flips) * per
        for part in range(per):
            samples[at + (1 + part)] = piece[:, part * BLOCK : (part + 1) * BLOCK]
    before = samples[0:blocks].reshape(blocks * channels, BLOCK)
    current = samples[1 : blocks + 1].reshape(blocks * channels, BLOCK)
    window = jnp.concatenate([before, current], 1)
    spec[0:per] = jnp.zeros((per,) + spec.shape[1:], F32)
    spec[per:] = (dot(window, table_high[...]) + dot(window, table_low[...])).reshape((blocks,) + spec.shape[1:])
    taps = filt.shape[0]
    packed = lax.broadcasted_iota(jnp.int32, (8, BLOCK), 1) == 0

    def group(g, carry):
        at = pl.ds(pl.multiple_of(g * 8, 8), 8)

        def load(ref, index):
            real, imag = ref[index, at, :BLOCK], ref[index, at, BLOCK:]
            return real, imag, real + imag

        for place in range(pieces):
            first = 2 * per * place + per
            count = min(first + per, taps)
            sums = [None] * per
            held = [load(spec, side * per + (first + q)) for q in range(per)]
            for j in range(count):
                taken = load(filt, j)
                for q in range(per):
                    if j <= first + q:
                        terms = tuple(x * f for x, f in zip(held[q], taken))
                        sums[q] = terms if sums[q] is None else tuple(s + t for s, t in zip(sums[q], terms))
                if j + 1 < count:
                    below = [load(spec, side * per + (first - j - 1))] if j < first else [None]
                    held = below + held[:-1]
            for q, (real, imag, both) in enumerate(sums):
                total[per * place + q, at, :BLOCK] = real - jnp.where(packed, 0.0, imag)
                total[per * place + q, at, BLOCK:] = jnp.where(packed, imag, both - real - imag)
        return carry

    lax.fori_loop(0, channels // 8, group, 0)
    sums = total[...].reshape(-1, 2 * BLOCK)
    high = sums.astype(BF16)
    low = (sums - high.astype(F32)).astype(BF16)
    conv = dot(high, back_high[...]) + dot(low, back_high[...]) + dot(high, back_low[...])
    result[...] = conv.astype(BF16).reshape(result.shape)
    for k, out in enumerate(outs):
        at = lax.bitwise_xor(me // 2, k) * per
        out[...] = jnp.concatenate([result[at + part] for part in range(per)], 1)


def mix_kernel(pieces, signal, gate, skip, *refs):
    ins, (keep_out, send_out, conv) = refs[:pieces], refs[pieces:]
    place = lax.axis_index("seq") // 2
    core = lax.rem(lax.axis_index("head"), 2)
    for k in range(pieces):
        conv[lax.bitwise_xor(place, k)] = ins[k][...]
    turned = conv[...].reshape(-1, conv.shape[-1]).T.astype(F32)
    mixed = (gate[...].astype(F32) * (turned + skip[...] * signal[...].astype(F32))).astype(BF16)
    half = keep_out.shape[0]
    low, high = mixed[:half], mixed[half:]
    keep_out[...] = jnp.where(core == 0, low, high)
    send_out[...] = jnp.where(core == 0, high, low)


def project_kernel(flips, own, other, own_w, other_w, *outs):
    head = lax.axis_index("head")
    width = outs[0].shape[1]
    for flip, out in zip(flips, outs):
        columns = pl.ds(pl.multiple_of(lax.bitwise_xor(head, flip) * width, width), width)
        terms = dot(own[...], own_w[:, columns]) + dot(other[...], other_w[:, columns])
        out[...] = terms.astype(out.dtype)


def sum_kernel(own, a, b, c, out):
    core = lax.rem(lax.axis_index("head"), 2)
    half = own.shape[0]
    here = own[...] + a[...].astype(F32)
    there = c[...].astype(F32) + b[...].astype(F32)
    out[pl.ds(pl.multiple_of(core * half, half), half), :] = here.astype(BF16)
    out[pl.ds(pl.multiple_of((1 - core) * half, half), half), :] = there.astype(BF16)


def turn_kernel(pieces, signal, *outs):
    outs, (held, sems) = outs[:pieces], outs[pieces:]
    place = lax.axis_index("seq") // 2
    share = outs[0].shape[0]
    order = [*range(1, pieces), 0]
    starts = [pl.multiple_of(lax.bitwise_xor(place, k) * share, share) for k in order]
    copies = fetch([signal.at[:, pl.ds(at, share)] for at in starts], [held.at[n] for n in range(pieces)], sems)
    for n, k in enumerate(order):
        copies[n].wait()
        outs[k][...] = held[n].T


def call(kernel, outs, *args, scratch=(), flops=0, grant=12, hbm=()):
    spaces = [pltpu.HBM if n in hbm else VMEM for n in range(len(args))]
    run = pl.pallas_call(
        kernel,
        out_shape=outs,
        in_specs=[pl.BlockSpec(memory_space=space) for space in spaces],
        out_specs=jax.tree.map(lambda _: pl.BlockSpec(memory_space=VMEM), outs),
        scratch_shapes=list(scratch),
        cost_estimate=pl.CostEstimate(flops=flops, bytes_accessed=0, transcendentals=0),
        compiler_params=pltpu.CompilerParams(vmem_limit_bytes=grant << 20),
    )
    args = [
        pltpu.with_memory_space_constraint(arg, pltpu.HBM) if n in hbm else arg
        for n, arg in enumerate(args)
    ]
    return run(*args)


def shape(dims, dtype=BF16):
    return jax.ShapeDtypeStruct(dims, dtype)


def flip(x, axis, by):
    size = lax.axis_size(axis)
    return lax.ppermute(x, axis, [(i, i ^ by) for i in range(size)])


def spread(signal, gate, skip, w_first, b_first, freq, w_mid, w_last, rate, out_w):
    length_local, channels = signal.shape
    ranks, heads = lax.axis_size("seq"), lax.axis_size("head")
    pieces = ranks // 2
    share = channels // pieces
    per = length_local // BLOCK
    blocks = ranks * per
    taps = K // BLOCK
    half = length_local // 2
    width = out_w.shape[1] // heads
    row = lambda v: v.reshape(1, -1)

    piece = shape((share, length_local))
    own = call(
        functools.partial(turn_kernel, pieces),
        (piece,) * pieces,
        signal,
        scratch=[pltpu.VMEM((pieces, length_local, share), BF16), pltpu.SemaphoreType.DMA((pieces,))],
        hbm=(0,),
    )
    parts = []
    for k in range(pieces):
        part = flip(own[k], "seq", 2 * k) if k else own[0]
        parts += [part, flip(part, "seq", 1)]

    forward_high, forward_low = split(forward_table())
    back_high, back_low = split(backward_table())
    filter_table = np.concatenate([forward_high[:BLOCK], forward_low[:BLOCK]], 0)
    operands = (jnp.asarray(feature_table()), w_first, row(b_first), row(freq), w_mid)
    hidden = call(
        functools.partial(hidden_kernel, len(operands)),
        shape((w_mid.shape[1], K), F32),
        *operands,
        scratch=[pltpu.VMEM(v.shape, v.dtype) for v in operands]
        + [pltpu.SemaphoreType.DMA((len(operands),))],
        flops=1_000_000_000,
        hbm=range(len(operands)),
    )
    operands = (w_last, row(rate), jnp.asarray(filter_table))
    filt = call(
        functools.partial(filter_kernel, len(operands)),
        shape((taps, share, 2 * BLOCK), F32),
        hidden,
        *operands,
        scratch=[pltpu.VMEM(v.shape, v.dtype) for v in operands]
        + [pltpu.SemaphoreType.DMA((len(operands),))],
        flops=2_000_000_000,
        hbm=range(1, 1 + len(operands)),
    )
    other_w = flip(out_w, "head", 1)
    convs = call(
        functools.partial(conv_kernel, pieces),
        (piece,) * pieces,
        filt,
        forward_high,
        forward_low,
        back_high,
        back_low,
        *parts,
        scratch=[
            pltpu.VMEM((blocks + 1, share, BLOCK), BF16),
            pltpu.VMEM((per + blocks, share, 2 * BLOCK), F32),
            pltpu.VMEM((blocks // 2, share, 2 * BLOCK), F32),
            pltpu.VMEM((blocks // 2, share, BLOCK), BF16),
        ],
        flops=3_000_000_000,
    )

    convs = [flip(conv, "seq", 2 * k) if k else conv for k, conv in enumerate(convs)]
    mixed = shape((half, channels))
    keep, send = call(
        functools.partial(mix_kernel, pieces),
        (mixed, mixed),
        signal,
        gate,
        row(skip),
        *convs,
        scratch=[pltpu.VMEM((pieces, share, length_local), BF16)],
        flops=500_000_000,
    )
    received = flip(send, "head", 1)
    terms, wide = shape((half, width)), shape((half, width), F32)
    factors = (keep, received, out_w, other_w)
    a, b = call(functools.partial(project_kernel, (2, 3)), (terms, terms), *factors, flops=500_000_000)
    a, b = flip(a, "head", 2), flip(b, "head", 3)
    c, here = call(functools.partial(project_kernel, (1, 0)), (wide, wide), *factors, flops=500_000_000)
    c = flip(c, "head", 1)
    return call(sum_kernel, shape((length_local, width)), here, a, b, c)


def shifted(x, axis, by):
    size = lax.axis_size(axis)
    pairs = [(i, i + by) for i in range(size) if 0 <= i + by < size]
    return lax.ppermute(x, axis, pairs)


def make_filter(w_first, b_first, freq, w_mid, w_last, rate, count):
    position = jnp.arange(count).astype(jnp.float32)
    bands = jnp.arange(1, BANDS + 1).astype(jnp.float32)
    angles = 2.0 * math.pi * position[:, None] * bands[None, :] / K
    features = jnp.concatenate([position[:, None] / K, jnp.cos(angles), jnp.sin(angles)], 1)
    first = jnp.sin(freq * (jnp.dot(features, w_first, precision=HIGHEST) + b_first))
    second = jnp.sin(freq * jnp.dot(first, w_mid, precision=HIGHEST))
    raw = jnp.dot(second, w_last, precision=HIGHEST)
    return (raw * jnp.exp(-rate[None, :] * position[:, None])).astype(jnp.bfloat16)


def transform_tables(block):
    doubled = 2 * block
    taps = jnp.arange(block)
    freqs = jnp.arange(block)
    outputs = jnp.arange(doubled)
    scale_angle = 2.0 * math.pi / doubled
    phase = (freqs[:, None] * taps[None, :] % doubled).astype(jnp.float32) * scale_angle
    alternate = (1 - 2 * (taps % 2)).astype(jnp.float32)
    forward_real = jnp.cos(phase)
    forward_imag = jnp.where(freqs[:, None] == 0, alternate[None, :], -jnp.sin(phase))
    phase_back = (outputs[:, None] * freqs[None, :] % doubled).astype(jnp.float32) * scale_angle
    alternate_back = (1 - 2 * (outputs % 2)).astype(jnp.float32)
    weights = jnp.where(freqs == 0, 1.0, 2.0).astype(jnp.float32)
    back_real = weights[None, :] * jnp.cos(phase_back) / doubled
    back_imag = (
        jnp.where(freqs[None, :] == 0, alternate_back[:, None], -2.0 * jnp.sin(phase_back))
        / doubled
    )
    return (forward_real, forward_imag, back_real, back_imag)


def long_convolve(padded, filt, length_local):
    channels = padded.shape[1]
    block = min(128, length_local)
    segments = K // block
    out_blocks = length_local // block
    in_blocks = padded.shape[0] // block
    forward_real, forward_imag, back_real, back_imag = transform_tables(block)
    values = padded.astype(jnp.float32).reshape(in_blocks, block, channels)
    kernels = filt.astype(jnp.float32).reshape(segments, block, channels)[::-1]
    spec_real = jnp.einsum("ft,ntc->nfc", forward_real, values, precision=HIGHEST)
    spec_imag = jnp.einsum("ft,ntc->nfc", forward_imag, values, precision=HIGHEST)
    kern_real = jnp.einsum("ft,ntc->nfc", forward_real, kernels, precision=HIGHEST)
    kern_imag = jnp.einsum("ft,ntc->nfc", forward_imag, kernels, precision=HIGHEST)
    upper = (jnp.arange(block) >= 1).astype(jnp.float32)[:, None]
    sums_real = []
    sums_imag = []
    for index in range(out_blocks + 1):
        window_real = spec_real[index : index + segments]
        window_imag = spec_imag[index : index + segments]
        both_imag = kern_imag * window_imag
        sums_real.append(jnp.sum(kern_real * window_real - upper * both_imag, 0))
        cross = kern_real * window_imag + kern_imag * window_real
        sums_imag.append(jnp.sum(upper * cross + (1.0 - upper) * both_imag, 0))
    total_real = jnp.stack(sums_real, 0)
    total_imag = jnp.stack(sums_imag, 0)
    pieces = jnp.einsum("tf,kfc->ktc", back_real, total_real, precision=HIGHEST)
    pieces = pieces + jnp.einsum("tf,kfc->ktc", back_imag, total_imag, precision=HIGHEST)
    joined = pieces[1:, :block] + pieces[:-1, block:]
    return joined.reshape(length_local, channels)


def halo(signal, gate, skip, w_first, b_first, freq, w_mid, w_last, rate, out_w):
    length_local, _ = signal.shape
    filt = make_filter(w_first, b_first, freq, w_mid, w_last, rate, K)
    reach = K // length_local
    earlier = [shifted(signal, "seq", step) for step in range(reach, 0, -1)]
    padded = jnp.concatenate(earlier + [signal], 0)
    conv = long_convolve(padded, filt, length_local)
    mixed = (gate.astype(jnp.float32) * (conv + skip[None, :] * signal.astype(jnp.float32))).astype(
        jnp.bfloat16
    )
    terms = jnp.dot(mixed, out_w, preferred_element_type=jnp.float32)
    result = lax.psum_scatter(terms, "head", scatter_dimension=1, tiled=True)
    return result.astype(jnp.bfloat16)


def local(signal, *rest):
    ranks, heads = lax.axis_size("seq"), lax.axis_size("head")
    length_local, channels = signal.shape
    small = ranks == 8 and ranks * length_local <= K and heads == 4 and length_local == 2 * BLOCK
    if small and channels == 128 * (ranks // 2):
        return spread(signal, *rest)
    return halo(signal, *rest)


def solution(mesh):
    placed = (
        P("seq", "head"),
        P("seq", "head"),
        P("head"),
        P(),
        P(),
        P(),
        P(),
        P(None, "head"),
        P("head"),
        P("head", None),
    )


    return jax.shard_map(
        local, mesh=mesh, in_specs=placed, out_specs=P("seq", "head"), check_vma=False
    )
```

```python
import functools
import math

import jax
import jax.numpy as jnp
import numpy as np
from jax import lax
from jax.experimental import pallas as pl
from jax.experimental.pallas import tpu as pltpu
from jax.sharding import PartitionSpec as P


K = 2048
BANDS = 16
BLOCK = 128
TILE = 16
VMEM = pltpu.MemorySpace.VMEM
BF16 = jnp.bfloat16
F32 = jnp.float32
HIGHEST = lax.Precision.HIGHEST


def feature_table():
    taps = np.arange(K, dtype=np.float64)
    bands = np.arange(1, BANDS + 1, dtype=np.float64)
    angles = 2.0 * np.pi * ((taps[None, :] * bands[:, None]) % K) / K
    features = np.concatenate([taps[None, :] / K, np.cos(angles), np.sin(angles)], 0)
    features = np.pad(features, ((0, -len(features) % TILE), (0, 0)))
    high, low = split(features)
    return np.concatenate([high, low, high], 0)


def split(table):
    table = np.asarray(table, np.float32)
    high = table.astype(BF16)
    low = (table - high.astype(np.float32)).astype(BF16)
    return high, low


def forward_table():
    size = 2 * BLOCK
    samples = np.arange(size)
    freqs = np.arange(BLOCK)
    phase = 2.0 * np.pi * ((samples[:, None] * freqs[None, :]) % size) / size
    real = np.cos(phase)
    imag = -np.sin(phase)
    imag[:, 0] = 1.0 - 2.0 * (samples % 2)
    return np.concatenate([real, imag], 1)


def backward_table():
    size = 2 * BLOCK
    samples = np.arange(BLOCK, size)
    freqs = np.arange(BLOCK)
    phase = 2.0 * np.pi * ((freqs[:, None] * samples[None, :]) % size) / size
    real = 2.0 * np.cos(phase)
    imag = -2.0 * np.sin(phase)
    real[0] = 1.0
    imag[0] = 1.0 - 2.0 * (samples % 2)
    return np.concatenate([real, imag], 0) / size


def dot(a, b):
    return jnp.dot(a, b, preferred_element_type=F32)


def sine(x):
    turns = jnp.round(x * (1.0 / math.pi))
    r = x - turns * 3.140625
    r = r - turns * 9.676535897932e-4
    odd = turns - 2.0 * jnp.floor(turns * 0.5)
    sign = 1.0 - 2.0 * odd
    s = r * r
    p = -2.5052108385e-8
    p = p * s + 2.7557319224e-6
    p = p * s - 1.9841269841e-4
    p = p * s + 8.3333333333e-3
    p = p * s - 1.6666666667e-1
    return sign * (r + r * (s * p))


def column(row):
    n = row.shape[1]
    square = (n, n)
    diagonal = lax.broadcasted_iota(jnp.int32, square, 0) == lax.broadcasted_iota(jnp.int32, square, 1)
    return jnp.sum(jnp.where(diagonal, jnp.broadcast_to(row, square), 0.0), 1, keepdims=True)


def parts_of(x):
    high = x.astype(BF16)
    return high, (x - high.astype(F32)).astype(BF16)


def dot_first(a, b):
    return lax.dot_general(a, b, (((0,), (0,)), ((), ())), preferred_element_type=F32)


def stack_left(x):
    high, low = parts_of(x)
    return jnp.concatenate([high, high, low], 0)


def stack_right(x):
    high, low = parts_of(x)
    return jnp.concatenate([high, low, high], 0)


def fetch(sources, targets, sems):
    copies = [
        pltpu.make_async_copy(source, target, sems.at[n])
        for n, (source, target) in enumerate(zip(sources, targets))
    ]
    for copy in copies:
        copy.start()
    return copies


def hidden_kernel(feat, w_first, bias, freq, w_mid, out, left):
    freqs = column(freq[...])
    high, low = parts_of(w_first[...])
    count = high.shape[0]
    rows = left.shape[0] // 3
    left[...] = jnp.zeros(left.shape, BF16)
    for n, part in enumerate((high, high, low)):
        left[n * rows : n * rows + count, :] = part
    first = sine(freqs * (dot_first(left[...], feat[...]) + column(bias[...])))
    second = sine(freqs * dot_first(stack_left(w_mid[...]), stack_right(first)))
    out[...] = stack_right(second)


def filter_kernel(hidden, w_last, rate, table_high, table_low, out):
    share = out.shape[1]
    own = pl.ds(pl.multiple_of((lax.axis_index("seq") // 2) * share, share), share)
    raw = dot_first(stack_left(w_last[:, own]), hidden[...])
    rates = column(rate[:, own])
    lane = lax.broadcasted_iota(jnp.int32, (1, BLOCK), 1).astype(F32)
    decay, step = jnp.exp(-rates * lane), jnp.exp(-rates * float(BLOCK))
    before = [jnp.zeros((share, BLOCK), BF16)]
    for j in range(out.shape[0]):
        before.append((raw[:, j * BLOCK : (j + 1) * BLOCK] * decay).astype(BF16))
        decay = decay * step
    window = jnp.concatenate([jnp.concatenate(before[:-1], 0), jnp.concatenate(before[1:], 0)], 1)
    out[...] = (dot(window, table_high[...]) + dot(window, table_low[...])).reshape(out.shape)


def conv_kernel(pieces, filt, table, back, *refs):
    ins, outs = refs[: 2 * pieces], refs[2 * pieces : 3 * pieces]
    spec, total, result = refs[3 * pieces :]
    me = lax.axis_index("seq")
    side = lax.rem(me, 2)
    channels = spec.shape[1]
    per = ins[0].shape[1] // BLOCK
    spec[0:per] = jnp.zeros((per,) + spec.shape[1:], F32)
    for flips, piece in enumerate(ins):
        at = lax.bitwise_xor(me, flips) * per + per
        for part in range(per):
            block = piece[:, part * BLOCK : (part + 1) * BLOCK]
            spec[at + part] = dot(jnp.concatenate([block, block], 1), table[...])
    taps = filt.shape[0]
    packed = lax.broadcasted_iota(jnp.int32, (8, BLOCK), 1) == 0

    def group(g, carry):
        at = pl.ds(pl.multiple_of(g * 8, 8), 8)

        def load(ref, index):
            real, imag = ref[index, at, :BLOCK], ref[index, at, BLOCK:]
            return real, imag, real + imag

        for place in range(pieces):
            first = 2 * per * place + per
            count = min(first + per, taps)
            sums = [None] * per
            held = [load(spec, side * per + (first + q)) for q in range(per)]
            for j in range(count):
                taken = load(filt, j)
                for q in range(per):
                    if j <= first + q:
                        terms = tuple(x * f for x, f in zip(held[q], taken))
                        sums[q] = terms if sums[q] is None else tuple(s + t for s, t in zip(sums[q], terms))
                if j + 1 < count:
                    below = [load(spec, side * per + (first - j - 1))] if j < first else [None]
                    held = below + held[:-1]
            for q, (real, imag, both) in enumerate(sums):
                total[per * place + q, at, :BLOCK] = real - jnp.where(packed, 0.0, imag)
                total[per * place + q, at, BLOCK:] = jnp.where(packed, imag, both - real - imag)
        return carry

    lax.fori_loop(0, channels // 8, group, 0)
    high, low = parts_of(total[...].reshape(-1, 2 * BLOCK))
    conv = dot(high, back[...])
    conv = conv[:, :BLOCK] + conv[:, BLOCK:] + dot(low, back[:, :BLOCK])
    result[...] = conv.astype(BF16).reshape(result.shape)
    for k, out in enumerate(outs):
        at = lax.bitwise_xor(me // 2, k) * per
        out[...] = jnp.concatenate([result[at + part] for part in range(per)], 1)


def mix_kernel(pieces, signal, gate, skip, *refs):
    ins, (keep_out, send_out, conv) = refs[:pieces], refs[pieces:]
    place = lax.axis_index("seq") // 2
    core = lax.rem(lax.axis_index("head"), 2)
    for k in range(pieces):
        conv[lax.bitwise_xor(place, k)] = ins[k][...]
    turned = conv[...].reshape(-1, conv.shape[-1]).T.astype(F32)
    mixed = (gate[...].astype(F32) * (turned + skip[...] * signal[...].astype(F32))).astype(BF16)
    half = keep_out.shape[0]
    low, high = mixed[:half], mixed[half:]
    keep_out[...] = jnp.where(core == 0, low, high)
    send_out[...] = jnp.where(core == 0, high, low)


def project_kernel(flips, own, other, own_w, other_w, *outs):
    head = lax.axis_index("head")
    width = outs[0].shape[1]
    for flip, out in zip(flips, outs):
        columns = pl.ds(pl.multiple_of(lax.bitwise_xor(head, flip) * width, width), width)
        terms = dot(own[...], own_w[:, columns]) + dot(other[...], other_w[:, columns])
        out[...] = terms.astype(out.dtype)


def sum_kernel(own, a, b, c, out):
    core = lax.rem(lax.axis_index("head"), 2)
    half = own.shape[0]
    here = own[...] + a[...].astype(F32)
    there = c[...].astype(F32) + b[...].astype(F32)
    out[pl.ds(pl.multiple_of(core * half, half), half), :] = here.astype(BF16)
    out[pl.ds(pl.multiple_of((1 - core) * half, half), half), :] = there.astype(BF16)


def turn_kernel(pieces, count, signal, *refs):
    others, outs, copied = refs[:count], refs[count : count + pieces], refs[count + pieces : 2 * count + pieces]
    held, sems = refs[2 * count + pieces :]
    place = lax.axis_index("seq") // 2
    share = outs[0].shape[0]
    order = [*range(1, pieces), 0]
    starts = [pl.multiple_of(lax.bitwise_xor(place, k) * share, share) for k in order]
    sources = [signal.at[:, pl.ds(at, share)] for at in starts]
    copies = fetch([*sources, *others], [*(held.at[n] for n in range(pieces)), *copied], sems)
    for n, k in enumerate(order):
        copies[n].wait()
        outs[k][...] = held[n].T
    for copy in copies[pieces:]:
        copy.wait()


def call(kernel, outs, *args, scratch=(), flops=0, grant=12, hbm=()):
    spaces = [pltpu.HBM if n in hbm else VMEM for n in range(len(args))]
    run = pl.pallas_call(
        kernel,
        out_shape=outs,
        in_specs=[pl.BlockSpec(memory_space=space) for space in spaces],
        out_specs=jax.tree.map(lambda _: pl.BlockSpec(memory_space=VMEM), outs),
        scratch_shapes=list(scratch),
        cost_estimate=pl.CostEstimate(flops=flops, bytes_accessed=0, transcendentals=0),
        compiler_params=pltpu.CompilerParams(vmem_limit_bytes=grant << 20),
    )
    args = [
        pltpu.with_memory_space_constraint(arg, pltpu.HBM) if n in hbm else arg
        for n, arg in enumerate(args)
    ]
    return run(*args)


def shape(dims, dtype=BF16):
    return jax.ShapeDtypeStruct(dims, dtype)


def flip(x, axis, by):
    size = lax.axis_size(axis)
    return lax.ppermute(x, axis, [(i, i ^ by) for i in range(size)])


def spread(signal, gate, skip, w_first, b_first, freq, w_mid, w_last, rate, out_w):
    length_local, channels = signal.shape
    ranks, heads = lax.axis_size("seq"), lax.axis_size("head")
    pieces = ranks // 2
    share = channels // pieces
    per = length_local // BLOCK
    blocks = ranks * per
    taps = K // BLOCK
    half = length_local // 2
    width = out_w.shape[1] // heads
    row = lambda v: v.reshape(1, -1)

    forward_high, forward_low = split(forward_table())
    block_table = np.concatenate([forward_high[:BLOCK], forward_low[:BLOCK]], 0)
    back_table = np.concatenate(split(backward_table()), 1)
    operands = (
        jnp.asarray(feature_table()),
        w_first,
        row(b_first),
        row(freq),
        w_mid,
        w_last,
        row(rate),
        jnp.asarray(forward_high),
        jnp.asarray(forward_low),
    )
    piece = shape((share, length_local))
    turned = call(
        functools.partial(turn_kernel, pieces, len(operands)),
        (piece,) * pieces + tuple(shape(v.shape, v.dtype) for v in operands),
        signal,
        *operands,
        scratch=[
            pltpu.VMEM((pieces, length_local, share), BF16),
            pltpu.SemaphoreType.DMA((pieces + len(operands),)),
        ],
        hbm=range(1 + len(operands)),
    )
    own, operands = turned[:pieces], turned[pieces:]
    parts = []
    for k in range(pieces):
        part = flip(own[k], "seq", 2 * k) if k else own[0]
        parts += [part, flip(part, "seq", 1)]

    hidden = call(
        hidden_kernel,
        shape((3 * w_mid.shape[1], K)),
        *operands[:5],
        scratch=[pltpu.VMEM((operands[0].shape[0], w_first.shape[1]), BF16)],
        flops=1_000_000_000,
    )
    filt = call(filter_kernel, shape((taps, share, 2 * BLOCK), F32), hidden, *operands[5:], flops=2_000_000_000)
    other_w = flip(out_w, "head", 1)
    convs = call(
        functools.partial(conv_kernel, pieces),
        (piece,) * pieces,
        filt,
        block_table,
        back_table,
        *parts,
        scratch=[
            pltpu.VMEM((per + blocks, share, 2 * BLOCK), F32),
            pltpu.VMEM((blocks // 2, share, 2 * BLOCK), F32),
            pltpu.VMEM((blocks // 2, share, BLOCK), BF16),
        ],
        flops=3_000_000_000,
    )

    convs = [flip(conv, "seq", 2 * k) if k else conv for k, conv in enumerate(convs)]
    mixed = shape((half, channels))
    keep, send = call(
        functools.partial(mix_kernel, pieces),
        (mixed, mixed),
        signal,
        gate,
        row(skip),
        *convs,
        scratch=[pltpu.VMEM((pieces, share, length_local), BF16)],
        flops=500_000_000,
    )
    received = flip(send, "head", 1)
    terms, wide = shape((half, width)), shape((half, width), F32)
    factors = (keep, received, out_w, other_w)
    a, b = call(functools.partial(project_kernel, (2, 3)), (terms, terms), *factors, flops=500_000_000)
    a, b = flip(a, "head", 2), flip(b, "head", 3)
    c, here = call(functools.partial(project_kernel, (1, 0)), (wide, wide), *factors, flops=500_000_000)
    c = flip(c, "head", 1)
    return call(sum_kernel, shape((length_local, width)), here, a, b, c)


def shifted(x, axis, by):
    size = lax.axis_size(axis)
    pairs = [(i, i + by) for i in range(size) if 0 <= i + by < size]
    return lax.ppermute(x, axis, pairs)


def make_filter(w_first, b_first, freq, w_mid, w_last, rate, count):
    position = jnp.arange(count).astype(jnp.float32)
    bands = jnp.arange(1, BANDS + 1).astype(jnp.float32)
    angles = 2.0 * math.pi * position[:, None] * bands[None, :] / K
    features = jnp.concatenate([position[:, None] / K, jnp.cos(angles), jnp.sin(angles)], 1)
    first = jnp.sin(freq * (jnp.dot(features, w_first, precision=HIGHEST) + b_first))
    second = jnp.sin(freq * jnp.dot(first, w_mid, precision=HIGHEST))
    raw = jnp.dot(second, w_last, precision=HIGHEST)
    return (raw * jnp.exp(-rate[None, :] * position[:, None])).astype(jnp.bfloat16)


def transform_tables(block):
    doubled = 2 * block
    taps = jnp.arange(block)
    freqs = jnp.arange(block)
    outputs = jnp.arange(doubled)
    scale_angle = 2.0 * math.pi / doubled
    phase = (freqs[:, None] * taps[None, :] % doubled).astype(jnp.float32) * scale_angle
    alternate = (1 - 2 * (taps % 2)).astype(jnp.float32)
    forward_real = jnp.cos(phase)
    forward_imag = jnp.where(freqs[:, None] == 0, alternate[None, :], -jnp.sin(phase))
    phase_back = (outputs[:, None] * freqs[None, :] % doubled).astype(jnp.float32) * scale_angle
    alternate_back = (1 - 2 * (outputs % 2)).astype(jnp.float32)
    weights = jnp.where(freqs == 0, 1.0, 2.0).astype(jnp.float32)
    back_real = weights[None, :] * jnp.cos(phase_back) / doubled
    back_imag = (
        jnp.where(freqs[None, :] == 0, alternate_back[:, None], -2.0 * jnp.sin(phase_back))
        / doubled
    )
    return (forward_real, forward_imag, back_real, back_imag)


def long_convolve(padded, filt, length_local):
    channels = padded.shape[1]
    block = min(128, length_local)
    segments = K // block
    out_blocks = length_local // block
    in_blocks = padded.shape[0] // block
    forward_real, forward_imag, back_real, back_imag = transform_tables(block)
    values = padded.astype(jnp.float32).reshape(in_blocks, block, channels)
    kernels = filt.astype(jnp.float32).reshape(segments, block, channels)[::-1]
    spec_real = jnp.einsum("ft,ntc->nfc", forward_real, values, precision=HIGHEST)
    spec_imag = jnp.einsum("ft,ntc->nfc", forward_imag, values, precision=HIGHEST)
    kern_real = jnp.einsum("ft,ntc->nfc", forward_real, kernels, precision=HIGHEST)
    kern_imag = jnp.einsum("ft,ntc->nfc", forward_imag, kernels, precision=HIGHEST)
    upper = (jnp.arange(block) >= 1).astype(jnp.float32)[:, None]
    sums_real = []
    sums_imag = []
    for index in range(out_blocks + 1):
        window_real = spec_real[index : index + segments]
        window_imag = spec_imag[index : index + segments]
        both_imag = kern_imag * window_imag
        sums_real.append(jnp.sum(kern_real * window_real - upper * both_imag, 0))
        cross = kern_real * window_imag + kern_imag * window_real
        sums_imag.append(jnp.sum(upper * cross + (1.0 - upper) * both_imag, 0))
    total_real = jnp.stack(sums_real, 0)
    total_imag = jnp.stack(sums_imag, 0)
    pieces = jnp.einsum("tf,kfc->ktc", back_real, total_real, precision=HIGHEST)
    pieces = pieces + jnp.einsum("tf,kfc->ktc", back_imag, total_imag, precision=HIGHEST)
    joined = pieces[1:, :block] + pieces[:-1, block:]
    return joined.reshape(length_local, channels)


def halo(signal, gate, skip, w_first, b_first, freq, w_mid, w_last, rate, out_w):
    length_local, _ = signal.shape
    filt = make_filter(w_first, b_first, freq, w_mid, w_last, rate, K)
    reach = K // length_local
    earlier = [shifted(signal, "seq", step) for step in range(reach, 0, -1)]
    padded = jnp.concatenate(earlier + [signal], 0)
    conv = long_convolve(padded, filt, length_local)
    mixed = (gate.astype(jnp.float32) * (conv + skip[None, :] * signal.astype(jnp.float32))).astype(
        jnp.bfloat16
    )
    terms = jnp.dot(mixed, out_w, preferred_element_type=jnp.float32)
    result = lax.psum_scatter(terms, "head", scatter_dimension=1, tiled=True)
    return result.astype(jnp.bfloat16)


def local(signal, *rest):
    ranks, heads = lax.axis_size("seq"), lax.axis_size("head")
    length_local, channels = signal.shape
    small = ranks == 8 and ranks * length_local <= K and heads == 4 and length_local == 2 * BLOCK
    if small and channels == 128 * (ranks // 2):
        return spread(signal, *rest)
    return halo(signal, *rest)


def solution(mesh):
    placed = (
        P("seq", "head"),
        P("seq", "head"),
        P("head"),
        P(),
        P(),
        P(),
        P(),
        P(None, "head"),
        P("head"),
        P("head", None),
    )


    return jax.shard_map(
        local, mesh=mesh, in_specs=placed, out_specs=P("seq", "head"), check_vma=False
    )
```

```python
import functools
import math

import jax
import jax.numpy as jnp
import numpy as np
from jax import lax
from jax.experimental import pallas as pl
from jax.experimental.pallas import tpu as pltpu
from jax.sharding import PartitionSpec as P


K = 2048
BANDS = 16
BLOCK = 128
TILE = 16
VMEM = pltpu.MemorySpace.VMEM
BF16 = jnp.bfloat16
F32 = jnp.float32
HIGHEST = lax.Precision.HIGHEST


def feature_table():
    taps = np.arange(K, dtype=np.float64)
    bands = np.arange(1, BANDS + 1, dtype=np.float64)
    angles = 2.0 * np.pi * ((taps[None, :] * bands[:, None]) % K) / K
    features = np.concatenate([taps[None, :] / K, np.cos(angles), np.sin(angles)], 0)
    features = np.pad(features, ((0, -len(features) % TILE), (0, 0)))
    high, low = split(features)
    return np.concatenate([high, low, high], 0)


def split(table):
    table = np.asarray(table, np.float32)
    high = table.astype(BF16)
    low = (table - high.astype(np.float32)).astype(BF16)
    return high, low


def forward_table():
    size = 2 * BLOCK
    samples = np.arange(size)
    freqs = np.arange(BLOCK)
    phase = 2.0 * np.pi * ((samples[:, None] * freqs[None, :]) % size) / size
    real = np.cos(phase)
    imag = -np.sin(phase)
    imag[:, 0] = 1.0 - 2.0 * (samples % 2)
    return np.concatenate([real, imag], 1)


def backward_table():
    size = 2 * BLOCK
    samples = np.arange(BLOCK, size)
    freqs = np.arange(BLOCK)
    phase = 2.0 * np.pi * ((freqs[:, None] * samples[None, :]) % size) / size
    real = 2.0 * np.cos(phase)
    imag = -2.0 * np.sin(phase)
    real[0] = 1.0
    imag[0] = 1.0 - 2.0 * (samples % 2)
    return np.concatenate([real, imag], 0) / size


def dot(a, b):
    return jnp.dot(a, b, preferred_element_type=F32)


def sine(x):
    turns = jnp.round(x * (1.0 / math.pi))
    r = x - turns * 3.140625
    r = r - turns * 9.676535897932e-4
    odd = turns - 2.0 * jnp.floor(turns * 0.5)
    sign = 1.0 - 2.0 * odd
    s = r * r
    p = -2.5052108385e-8
    p = p * s + 2.7557319224e-6
    p = p * s - 1.9841269841e-4
    p = p * s + 8.3333333333e-3
    p = p * s - 1.6666666667e-1
    return sign * (r + r * (s * p))


def column(row):
    n = row.shape[1]
    square = (n, n)
    diagonal = lax.broadcasted_iota(jnp.int32, square, 0) == lax.broadcasted_iota(jnp.int32, square, 1)
    return jnp.sum(jnp.where(diagonal, jnp.broadcast_to(row, square), 0.0), 1, keepdims=True)


def parts_of(x):
    high = x.astype(BF16)
    return high, (x - high.astype(F32)).astype(BF16)


def dot_first(a, b):
    return lax.dot_general(a, b, (((0,), (0,)), ((), ())), preferred_element_type=F32)


def stack_left(x):
    high, low = parts_of(x)
    return jnp.concatenate([high, high, low], 0)


def stack_right(x):
    high, low = parts_of(x)
    return jnp.concatenate([high, low, high], 0)


def fetch(sources, targets, sems):
    copies = [
        pltpu.make_async_copy(source, target, sems.at[n])
        for n, (source, target) in enumerate(zip(sources, targets))
    ]
    for copy in copies:
        copy.start()
    return copies


def hidden_kernel(feat, w_first, bias, freq, w_mid, out, left):
    freqs = column(freq[...])
    high, low = parts_of(w_first[...])
    count = high.shape[0]
    rows = left.shape[0] // 3
    left[...] = jnp.zeros(left.shape, BF16)
    for n, part in enumerate((high, high, low)):
        left[n * rows : n * rows + count, :] = part
    first = sine(freqs * (dot_first(left[...], feat[...]) + column(bias[...])))
    second = sine(freqs * dot_first(stack_left(w_mid[...]), stack_right(first)))
    out[...] = stack_right(second)


def filter_kernel(hidden, w_last, rate, table_high, table_low, out):
    share = out.shape[1]
    own = pl.ds(pl.multiple_of((lax.axis_index("seq") // 2) * share, share), share)
    raw = dot_first(stack_left(w_last[:, own]), hidden[...])
    rates = column(rate[:, own])
    lane = lax.broadcasted_iota(jnp.int32, (1, BLOCK), 1).astype(F32)
    decay, step = jnp.exp(-rates * lane), jnp.exp(-rates * float(BLOCK))
    before = [jnp.zeros((share, BLOCK), BF16)]
    for j in range(out.shape[0]):
        before.append((raw[:, j * BLOCK : (j + 1) * BLOCK] * decay).astype(BF16))
        decay = decay * step
    window = jnp.concatenate([jnp.concatenate(before[:-1], 0), jnp.concatenate(before[1:], 0)], 1)
    out[...] = (dot(window, table_high[...]) + dot(window, table_low[...])).reshape(out.shape)


def spectra(pieces, spec, first, flips, table):
    place = lax.axis_index("seq") // 2
    per = pieces[0].shape[1] // BLOCK
    for flip, piece in zip(flips, pieces):
        at = (lax.bitwise_xor(place, flip) + first) * per
        for part in range(per):
            block = piece[:, part * BLOCK : (part + 1) * BLOCK]
            spec[at + part] = dot(jnp.concatenate([block, block], 1), table[...])


def products(filt, spec, places, per, shift, apart, done):
    taps = filt.shape[0]
    packed = lax.broadcasted_iota(jnp.int32, (8, BLOCK), 1) == 0

    def group(g, carry):
        at = pl.ds(pl.multiple_of(g * 8, 8), 8)

        def load(ref, index):
            real, imag = ref[index, at, :BLOCK], ref[index, at, BLOCK:]
            return real, imag, real + imag

        for place in range(places):
            sums = [None] * per
            for d in range(place + 1):
                held = [load(spec, (place - d + shift) * per + r) for r in range(per)]
                windows = {}
                for q in range(per):
                    for r in range(per):
                        j = 2 * per * d + apart + q - r
                        if 0 <= j < taps:
                            if j not in windows:
                                windows[j] = load(filt, j)
                            terms = tuple(x * f for x, f in zip(held[r], windows[j]))
                            sums[q] = terms if sums[q] is None else tuple(s + t for s, t in zip(sums[q], terms))
            for q, (real, imag, both) in enumerate(sums):
                done(
                    per * place + q,
                    at,
                    real - jnp.where(packed, 0.0, imag),
                    jnp.where(packed, imag, both - real - imag),
                )
        return carry

    lax.fori_loop(0, spec.shape[1] // 8, group, 0)


def own_kernel(pieces, filt, table, *refs):
    ins, out, spec = refs[:pieces], refs[pieces], refs[pieces + 1]
    per = ins[0].shape[1] // BLOCK
    spectra(ins, spec, 0, range(pieces), table)

    def done(block, at, real, imag):
        out[block, at, :BLOCK] = real
        out[block, at, BLOCK:] = imag

    products(filt, spec, pieces, per, 0, 0, done)


def conv_kernel(pieces, filt, table, back, own, *refs):
    ins, outs = refs[:pieces], refs[pieces : 2 * pieces]
    spec, total, result = refs[2 * pieces :]
    me = lax.axis_index("seq")
    per = ins[0].shape[1] // BLOCK
    spec[0:per] = jnp.zeros((per,) + spec.shape[1:], F32)
    spectra(ins, spec, 1, range(pieces), table)

    def done(block, at, real, imag):
        total[block, at, :BLOCK] = own[block, at, :BLOCK] + real
        total[block, at, BLOCK:] = own[block, at, BLOCK:] + imag

    products(filt, spec, pieces, per, lax.rem(me, 2), per, done)
    high, low = parts_of(total[...].reshape(-1, 2 * BLOCK))
    conv = dot(high, back[...])
    conv = conv[:, :BLOCK] + conv[:, BLOCK:] + dot(low, back[:, :BLOCK])
    result[...] = conv.astype(BF16).reshape(result.shape)
    for k, out in enumerate(outs):
        at = lax.bitwise_xor(me // 2, k) * per
        out[...] = jnp.concatenate([result[at + part] for part in range(per)], 1)


def mix_kernel(pieces, signal, gate, skip, *refs):
    ins, (keep_out, send_out, conv) = refs[:pieces], refs[pieces:]
    place = lax.axis_index("seq") // 2
    core = lax.rem(lax.axis_index("head"), 2)
    for k in range(pieces):
        conv[lax.bitwise_xor(place, k)] = ins[k][...]
    turned = conv[...].reshape(-1, conv.shape[-1]).T.astype(F32)
    mixed = (gate[...].astype(F32) * (turned + skip[...] * signal[...].astype(F32))).astype(BF16)
    half = keep_out.shape[0]
    low, high = mixed[:half], mixed[half:]
    keep_out[...] = jnp.where(core == 0, low, high)
    send_out[...] = jnp.where(core == 0, high, low)


def project_kernel(flips, own, other, own_w, other_w, *outs):
    head = lax.axis_index("head")
    width = outs[0].shape[1]
    for flip, out in zip(flips, outs):
        columns = pl.ds(pl.multiple_of(lax.bitwise_xor(head, flip) * width, width), width)
        terms = dot(own[...], own_w[:, columns]) + dot(other[...], other_w[:, columns])
        out[...] = terms.astype(out.dtype)


def sum_kernel(other_half, first, second, *refs):
    out, held, sem = refs[-3:]
    half = held.shape[0]
    part = lax.bitwise_xor(lax.rem(lax.axis_index("head"), 2), other_half)
    held[...] = (first[...].astype(F32) + second[...].astype(F32)).astype(BF16)
    rows = pl.ds(pl.multiple_of(part * half, half), half)
    copy = pltpu.make_async_copy(held, out.at[rows, :], sem)
    copy.start()
    copy.wait()


def add_half(other_half, out, first, second):
    fresh = isinstance(out, jax.ShapeDtypeStruct)
    half, width = first.shape
    run = pl.pallas_call(
        functools.partial(sum_kernel, other_half),
        out_shape=shape(out.shape),
        in_specs=[pl.BlockSpec(memory_space=VMEM)] * 2 + [pl.BlockSpec(memory_space=pltpu.HBM)] * (not fresh),
        out_specs=pl.BlockSpec(memory_space=pltpu.HBM),
        scratch_shapes=[pltpu.VMEM((half, width), BF16), pltpu.SemaphoreType.DMA(())],
        input_output_aliases={} if fresh else {2: 0},
        cost_estimate=pl.CostEstimate(flops=100_000_000, bytes_accessed=0, transcendentals=0),
        compiler_params=pltpu.CompilerParams(vmem_limit_bytes=4 << 20),
    )
    return run(first, second) if fresh else run(first, second, out)


def turn_kernel(pieces, count, signal, *refs):
    others, outs, copied = refs[:count], refs[count : count + pieces], refs[count + pieces : 2 * count + pieces]
    held, sems = refs[2 * count + pieces :]
    place = lax.axis_index("seq") // 2
    share = outs[0].shape[0]
    order = [*range(1, pieces), 0]
    starts = [pl.multiple_of(lax.bitwise_xor(place, k) * share, share) for k in order]
    sources = [signal.at[:, pl.ds(at, share)] for at in starts]
    copies = fetch([*sources, *others], [*(held.at[n] for n in range(pieces)), *copied], sems)
    for n, k in enumerate(order):
        copies[n].wait()
        outs[k][...] = held[n].T
    for copy in copies[pieces:]:
        copy.wait()


def call(kernel, outs, *args, scratch=(), flops=0, grant=12, hbm=()):
    spaces = [pltpu.HBM if n in hbm else VMEM for n in range(len(args))]
    run = pl.pallas_call(
        kernel,
        out_shape=outs,
        in_specs=[pl.BlockSpec(memory_space=space) for space in spaces],
        out_specs=jax.tree.map(lambda _: pl.BlockSpec(memory_space=VMEM), outs),
        scratch_shapes=list(scratch),
        cost_estimate=pl.CostEstimate(flops=flops, bytes_accessed=0, transcendentals=0),
        compiler_params=pltpu.CompilerParams(vmem_limit_bytes=grant << 20),
    )
    args = [
        pltpu.with_memory_space_constraint(arg, pltpu.HBM) if n in hbm else arg
        for n, arg in enumerate(args)
    ]
    return run(*args)


def shape(dims, dtype=BF16):
    return jax.ShapeDtypeStruct(dims, dtype)


def flip(x, axis, by):
    size = lax.axis_size(axis)
    return lax.ppermute(x, axis, [(i, i ^ by) for i in range(size)])


def spread(signal, gate, skip, w_first, b_first, freq, w_mid, w_last, rate, out_w):
    length_local, channels = signal.shape
    ranks, heads = lax.axis_size("seq"), lax.axis_size("head")
    pieces = ranks // 2
    share = channels // pieces
    per = length_local // BLOCK
    blocks = ranks * per
    taps = K // BLOCK
    half = length_local // 2
    width = out_w.shape[1] // heads
    row = lambda v: v.reshape(1, -1)

    forward_high, forward_low = split(forward_table())
    block_table = np.concatenate([forward_high[:BLOCK], forward_low[:BLOCK]], 0)
    back_table = np.concatenate(split(backward_table()), 1)
    operands = (
        jnp.asarray(feature_table()),
        w_first,
        row(b_first),
        row(freq),
        w_mid,
        w_last,
        row(rate),
        jnp.asarray(forward_high),
        jnp.asarray(forward_low),
    )
    piece = shape((share, length_local))
    turned = call(
        functools.partial(turn_kernel, pieces, len(operands)),
        (piece,) * pieces + tuple(shape(v.shape, v.dtype) for v in operands),
        signal,
        *operands,
        scratch=[
            pltpu.VMEM((pieces, length_local, share), BF16),
            pltpu.SemaphoreType.DMA((pieces + len(operands),)),
        ],
        hbm=range(1 + len(operands)),
    )
    own, operands = turned[:pieces], turned[pieces:]
    near = [flip(own[k], "seq", 2 * k) if k else own[0] for k in range(pieces)]
    beside = [flip(near[k], "seq", 1) for k in range(pieces)]

    hidden = call(
        hidden_kernel,
        shape((3 * w_mid.shape[1], K)),
        *operands[:5],
        scratch=[pltpu.VMEM((operands[0].shape[0], w_first.shape[1]), BF16)],
        flops=1_000_000_000,
    )
    filt = call(filter_kernel, shape((taps, share, 2 * BLOCK), F32), hidden, *operands[5:], flops=2_000_000_000)
    other_w = flip(out_w, "head", 1)
    sums = shape((blocks // 2, share, 2 * BLOCK), F32)
    early = call(
        functools.partial(own_kernel, pieces),
        sums,
        filt,
        block_table,
        *near,
        scratch=[pltpu.VMEM(sums.shape, F32)],
        flops=1_000_000_000,
    )
    convs = call(
        functools.partial(conv_kernel, pieces),
        (piece,) * pieces,
        filt,
        block_table,
        back_table,
        early,
        *beside,
        scratch=[
            pltpu.VMEM((per + blocks // 2, share, 2 * BLOCK), F32),
            pltpu.VMEM(sums.shape, F32),
            pltpu.VMEM((blocks // 2, share, BLOCK), BF16),
        ],
        flops=3_000_000_000,
    )

    convs = [flip(conv, "seq", 2 * k) if k else conv for k, conv in enumerate(convs)]
    mixed = shape((half, channels))
    keep, send = call(
        functools.partial(mix_kernel, pieces),
        (mixed, mixed),
        signal,
        gate,
        row(skip),
        *convs,
        scratch=[pltpu.VMEM((pieces, share, length_local), BF16)],
        flops=500_000_000,
    )
    received = flip(send, "head", 1)
    terms, wide = shape((half, width)), shape((half, width), F32)
    factors = (keep, received, out_w, other_w)

    def project(flips, outs):
        return call(functools.partial(project_kernel, flips), outs, *factors, flops=500_000_000)

    (a,) = project((2,), (terms,))
    a = flip(a, "head", 2)
    (b,) = project((3,), (terms,))
    b = flip(b, "head", 3)
    c, here = project((1, 0), (wide, wide))
    c = flip(c, "head", 1)
    out = add_half(0, shape((length_local, width)), here, a)
    return add_half(1, out, c, b)


def shifted(x, axis, by):
    size = lax.axis_size(axis)
    pairs = [(i, i + by) for i in range(size) if 0 <= i + by < size]
    return lax.ppermute(x, axis, pairs)


def make_filter(w_first, b_first, freq, w_mid, w_last, rate, count):
    position = jnp.arange(count).astype(jnp.float32)
    bands = jnp.arange(1, BANDS + 1).astype(jnp.float32)
    angles = 2.0 * math.pi * position[:, None] * bands[None, :] / K
    features = jnp.concatenate([position[:, None] / K, jnp.cos(angles), jnp.sin(angles)], 1)
    first = jnp.sin(freq * (jnp.dot(features, w_first, precision=HIGHEST) + b_first))
    second = jnp.sin(freq * jnp.dot(first, w_mid, precision=HIGHEST))
    raw = jnp.dot(second, w_last, precision=HIGHEST)
    return (raw * jnp.exp(-rate[None, :] * position[:, None])).astype(jnp.bfloat16)


def transform_tables(block):
    doubled = 2 * block
    taps = jnp.arange(block)
    freqs = jnp.arange(block)
    outputs = jnp.arange(doubled)
    scale_angle = 2.0 * math.pi / doubled
    phase = (freqs[:, None] * taps[None, :] % doubled).astype(jnp.float32) * scale_angle
    alternate = (1 - 2 * (taps % 2)).astype(jnp.float32)
    forward_real = jnp.cos(phase)
    forward_imag = jnp.where(freqs[:, None] == 0, alternate[None, :], -jnp.sin(phase))
    phase_back = (outputs[:, None] * freqs[None, :] % doubled).astype(jnp.float32) * scale_angle
    alternate_back = (1 - 2 * (outputs % 2)).astype(jnp.float32)
    weights = jnp.where(freqs == 0, 1.0, 2.0).astype(jnp.float32)
    back_real = weights[None, :] * jnp.cos(phase_back) / doubled
    back_imag = (
        jnp.where(freqs[None, :] == 0, alternate_back[:, None], -2.0 * jnp.sin(phase_back))
        / doubled
    )
    return (forward_real, forward_imag, back_real, back_imag)


def long_convolve(padded, filt, length_local):
    channels = padded.shape[1]
    block = min(128, length_local)
    segments = K // block
    out_blocks = length_local // block
    in_blocks = padded.shape[0] // block
    forward_real, forward_imag, back_real, back_imag = transform_tables(block)
    values = padded.astype(jnp.float32).reshape(in_blocks, block, channels)
    kernels = filt.astype(jnp.float32).reshape(segments, block, channels)[::-1]
    spec_real = jnp.einsum("ft,ntc->nfc", forward_real, values, precision=HIGHEST)
    spec_imag = jnp.einsum("ft,ntc->nfc", forward_imag, values, precision=HIGHEST)
    kern_real = jnp.einsum("ft,ntc->nfc", forward_real, kernels, precision=HIGHEST)
    kern_imag = jnp.einsum("ft,ntc->nfc", forward_imag, kernels, precision=HIGHEST)
    upper = (jnp.arange(block) >= 1).astype(jnp.float32)[:, None]
    sums_real = []
    sums_imag = []
    for index in range(out_blocks + 1):
        window_real = spec_real[index : index + segments]
        window_imag = spec_imag[index : index + segments]
        both_imag = kern_imag * window_imag
        sums_real.append(jnp.sum(kern_real * window_real - upper * both_imag, 0))
        cross = kern_real * window_imag + kern_imag * window_real
        sums_imag.append(jnp.sum(upper * cross + (1.0 - upper) * both_imag, 0))
    total_real = jnp.stack(sums_real, 0)
    total_imag = jnp.stack(sums_imag, 0)
    pieces = jnp.einsum("tf,kfc->ktc", back_real, total_real, precision=HIGHEST)
    pieces = pieces + jnp.einsum("tf,kfc->ktc", back_imag, total_imag, precision=HIGHEST)
    joined = pieces[1:, :block] + pieces[:-1, block:]
    return joined.reshape(length_local, channels)


def halo(signal, gate, skip, w_first, b_first, freq, w_mid, w_last, rate, out_w):
    length_local, _ = signal.shape
    filt = make_filter(w_first, b_first, freq, w_mid, w_last, rate, K)
    reach = K // length_local
    earlier = [shifted(signal, "seq", step) for step in range(reach, 0, -1)]
    padded = jnp.concatenate(earlier + [signal], 0)
    conv = long_convolve(padded, filt, length_local)
    mixed = (gate.astype(jnp.float32) * (conv + skip[None, :] * signal.astype(jnp.float32))).astype(
        jnp.bfloat16
    )
    terms = jnp.dot(mixed, out_w, preferred_element_type=jnp.float32)
    result = lax.psum_scatter(terms, "head", scatter_dimension=1, tiled=True)
    return result.astype(jnp.bfloat16)


def local(signal, *rest):
    ranks, heads = lax.axis_size("seq"), lax.axis_size("head")
    length_local, channels = signal.shape
    small = ranks == 8 and ranks * length_local <= K and heads == 4 and length_local == 2 * BLOCK
    if small and channels == 128 * (ranks // 2):
        return spread(signal, *rest)
    return halo(signal, *rest)


def solution(mesh):
    placed = (
        P("seq", "head"),
        P("seq", "head"),
        P("head"),
        P(),
        P(),
        P(),
        P(),
        P(None, "head"),
        P("head"),
        P("head", None),
    )


    return jax.shard_map(
        local, mesh=mesh, in_specs=placed, out_specs=P("seq", "head"), check_vma=False
    )
```

```python
import functools
import math

import jax
import jax.numpy as jnp
import numpy as np
from jax import lax
from jax.experimental import pallas as pl
from jax.experimental.pallas import tpu as pltpu
from jax.sharding import PartitionSpec as P


K = 2048
BANDS = 16
BLOCK = 128
TILE = 16
VMEM = pltpu.MemorySpace.VMEM
BF16 = jnp.bfloat16
F32 = jnp.float32
HIGHEST = lax.Precision.HIGHEST


def feature_table():
    taps = np.arange(K, dtype=np.float64)
    bands = np.arange(1, BANDS + 1, dtype=np.float64)
    angles = 2.0 * np.pi * ((taps[None, :] * bands[:, None]) % K) / K
    features = np.concatenate([taps[None, :] / K, np.cos(angles), np.sin(angles)], 0)
    features = np.pad(features, ((0, -len(features) % TILE), (0, 0)))
    return np.concatenate(split(features), 0)


def split(table):
    table = np.asarray(table, np.float32)
    high = table.astype(BF16)
    low = (table - high.astype(np.float32)).astype(BF16)
    return high, low


def forward_table():
    size = 2 * BLOCK
    samples = np.arange(size)
    freqs = np.arange(BLOCK)
    phase = 2.0 * np.pi * ((samples[:, None] * freqs[None, :]) % size) / size
    real = np.cos(phase)
    imag = -np.sin(phase)
    imag[:, 0] = 1.0 - 2.0 * (samples % 2)
    return np.concatenate([real, imag], 1)


def backward_table():
    size = 2 * BLOCK
    samples = np.arange(BLOCK, size)
    freqs = np.arange(BLOCK)
    phase = 2.0 * np.pi * ((freqs[:, None] * samples[None, :]) % size) / size
    real = 2.0 * np.cos(phase)
    imag = -2.0 * np.sin(phase)
    real[0] = 1.0
    imag[0] = 1.0 - 2.0 * (samples % 2)
    return np.concatenate([real, imag], 0) / size


def dot(a, b):
    return jnp.dot(a, b, preferred_element_type=F32)


SINE = (6.283182621, -41.34142303, 81.59618378, -76.58010101, 41.20539856, -12.27126789)


def sine(turns):
    r = turns - jnp.round(turns)
    s = r * r
    p = SINE[-1] * s + SINE[-2]
    for value in SINE[-3::-1]:
        p = p * s + value
    return p * r


def column(row):
    n = row.shape[1]
    square = (n, n)
    diagonal = lax.broadcasted_iota(jnp.int32, square, 0) == lax.broadcasted_iota(jnp.int32, square, 1)
    return jnp.sum(jnp.where(diagonal, jnp.broadcast_to(row, square), 0.0), 1, keepdims=True)


def parts_of(x):
    high = x.astype(BF16)
    return high, (x - high.astype(F32)).astype(BF16)


def dot_first(a, b):
    return lax.dot_general(a, b, (((0,), (0,)), ((), ())), preferred_element_type=F32)


def stack_left(x):
    high, low = parts_of(x)
    return jnp.concatenate([high, high, low], 0)


def stack_right(x):
    high, low = parts_of(x)
    return jnp.concatenate([high, low, high], 0)


def fetch(sources, targets, sems):
    copies = [
        pltpu.make_async_copy(source, target, sems.at[n])
        for n, (source, target) in enumerate(zip(sources, targets))
    ]
    for copy in copies:
        copy.start()
    return copies


def hidden_kernel(feat, w_first, bias, freq, w_mid, out, left):
    turns = column(freq[...] * (0.5 / math.pi))
    high, low = parts_of(w_first[...])
    count = high.shape[0]
    rows = left.shape[0] // 3
    left[...] = jnp.zeros(left.shape, BF16)
    for n, part in enumerate((high, high, low)):
        left[n * rows : n * rows + count, :] = part
    features = jnp.concatenate([feat[...], feat[:rows]], 0)
    first = sine(turns * (dot_first(left[...], features) + column(bias[...])))
    second = sine(turns * dot_first(stack_left(w_mid[...]), stack_right(first)))
    out[...] = stack_right(second)


def filter_kernel(hidden, w_last, rate, table_high, table_low, out):
    share = out.shape[1]
    own = pl.ds(pl.multiple_of((lax.axis_index("seq") // 2) * share, share), share)
    raw = dot_first(stack_left(w_last[:, own]), hidden[...])
    rates = column(rate[:, own])
    lane = lax.broadcasted_iota(jnp.int32, (1, BLOCK), 1).astype(F32)
    decay, step = jnp.exp(-rates * lane), jnp.exp(-rates * float(BLOCK))
    before = [jnp.zeros((share, BLOCK), BF16)]
    for j in range(out.shape[0]):
        before.append((raw[:, j * BLOCK : (j + 1) * BLOCK] * decay).astype(BF16))
        decay = decay * step
    window = jnp.concatenate([jnp.concatenate(before[:-1], 0), jnp.concatenate(before[1:], 0)], 1)
    out[...] = (dot(window, table_high[...]) + dot(window, table_low[...])).reshape(out.shape)


def spectra(pieces, spec, first, flips, table):
    place = lax.axis_index("seq") // 2
    per = pieces[0].shape[1] // BLOCK
    for flip, piece in zip(flips, pieces):
        at = (lax.bitwise_xor(place, flip) + first) * per
        for part in range(per):
            block = piece[:, part * BLOCK : (part + 1) * BLOCK]
            spec[at + part] = dot(jnp.concatenate([block, block], 1), table[...])


def products(filt, spec, places, per, shift, apart, done):
    taps = filt.shape[0]
    packed = lax.broadcasted_iota(jnp.int32, (8, BLOCK), 1) == 0

    def group(g, carry):
        at = pl.ds(pl.multiple_of(g * 8, 8), 8)

        def load(ref, index):
            real, imag = ref[index, at, :BLOCK], ref[index, at, BLOCK:]
            return real, imag, real + imag

        for place in range(places):
            sums = [None] * per
            for d in range(place + 1):
                held = [load(spec, (place - d + shift) * per + r) for r in range(per)]
                windows = {}
                for q in range(per):
                    for r in range(per):
                        j = 2 * per * d + apart + q - r
                        if 0 <= j < taps:
                            if j not in windows:
                                windows[j] = load(filt, j)
                            terms = tuple(x * f for x, f in zip(held[r], windows[j]))
                            sums[q] = terms if sums[q] is None else tuple(s + t for s, t in zip(sums[q], terms))
            for q, (real, imag, both) in enumerate(sums):
                done(
                    per * place + q,
                    at,
                    real - jnp.where(packed, 0.0, imag),
                    jnp.where(packed, imag, both - real - imag),
                )
        return carry

    lax.fori_loop(0, spec.shape[1] // 8, group, 0)


def own_kernel(pieces, filt, table, *refs):
    ins, out, spec = refs[:pieces], refs[pieces], refs[pieces + 1]
    per = ins[0].shape[1] // BLOCK
    spectra(ins, spec, 0, range(pieces), table)

    def done(block, at, real, imag):
        out[block, at, :BLOCK] = real
        out[block, at, BLOCK:] = imag

    products(filt, spec, pieces, per, 0, 0, done)


def conv_kernel(pieces, filt, table, back, own, *refs):
    ins, outs = refs[:pieces], refs[pieces : 2 * pieces]
    spec, total, result = refs[2 * pieces :]
    me = lax.axis_index("seq")
    per = ins[0].shape[1] // BLOCK
    spec[0:per] = jnp.zeros((per,) + spec.shape[1:], F32)
    spectra(ins, spec, 1, range(pieces), table)

    def done(block, at, real, imag):
        total[block, at, :BLOCK] = own[block, at, :BLOCK] + real
        total[block, at, BLOCK:] = own[block, at, BLOCK:] + imag

    products(filt, spec, pieces, per, lax.rem(me, 2), per, done)
    high, low = parts_of(total[...].reshape(-1, 2 * BLOCK))
    conv = dot(high, back[...])
    conv = conv[:, :BLOCK] + conv[:, BLOCK:] + dot(low, back[:, :BLOCK])
    result[...] = conv.astype(BF16).reshape(result.shape)
    for k, out in enumerate(outs):
        at = lax.bitwise_xor(me // 2, k) * per
        out[...] = jnp.concatenate([result[at + part] for part in range(per)], 1)


def mix_kernel(pieces, signal, gate, skip, *refs):
    ins, (keep_out, send_out, conv) = refs[:pieces], refs[pieces:]
    place = lax.axis_index("seq") // 2
    core = lax.rem(lax.axis_index("head"), 2)
    for k in range(pieces):
        conv[lax.bitwise_xor(place, k)] = ins[k][...]
    turned = conv[...].reshape(-1, conv.shape[-1]).T.astype(F32)
    mixed = (gate[...].astype(F32) * (turned + skip[...] * signal[...].astype(F32))).astype(BF16)
    half = keep_out.shape[0]
    low, high = mixed[:half], mixed[half:]
    keep_out[...] = jnp.where(core == 0, low, high)
    send_out[...] = jnp.where(core == 0, high, low)


def project_kernel(flips, own, weights, *outs):
    head = lax.axis_index("head")
    width = outs[0].shape[1]
    for flip, out in zip(flips, outs):
        columns = pl.ds(pl.multiple_of(lax.bitwise_xor(head, flip) * width, width), width)
        out[...] = dot(own[...], weights[:, columns])


def add_kernel(flips, other, weights, *refs):
    sums, outs = refs[: len(flips)], refs[len(flips) :]
    head = lax.axis_index("head")
    width = outs[0].shape[1]
    for flip, total, out in zip(flips, sums, outs):
        columns = pl.ds(pl.multiple_of(lax.bitwise_xor(head, flip) * width, width), width)
        out[...] = (total[...] + dot(other[...], weights[:, columns])).astype(out.dtype)


def sum_kernel(other_half, first, second, *refs):
    out, held, sem = refs[-3:]
    half = held.shape[0]
    part = lax.bitwise_xor(lax.rem(lax.axis_index("head"), 2), other_half)
    held[...] = (first[...].astype(F32) + second[...].astype(F32)).astype(BF16)
    rows = pl.ds(pl.multiple_of(part * half, half), half)
    copy = pltpu.make_async_copy(held, out.at[rows, :], sem)
    copy.start()
    copy.wait()


def add_half(other_half, out, first, second):
    fresh = isinstance(out, jax.ShapeDtypeStruct)
    half, width = first.shape
    run = pl.pallas_call(
        functools.partial(sum_kernel, other_half),
        out_shape=shape(out.shape),
        in_specs=[pl.BlockSpec(memory_space=VMEM)] * 2 + [pl.BlockSpec(memory_space=pltpu.HBM)] * (not fresh),
        out_specs=pl.BlockSpec(memory_space=pltpu.HBM),
        scratch_shapes=[pltpu.VMEM((half, width), BF16), pltpu.SemaphoreType.DMA(())],
        input_output_aliases={} if fresh else {2: 0},
        cost_estimate=pl.CostEstimate(flops=100_000_000, bytes_accessed=0, transcendentals=0),
        compiler_params=pltpu.CompilerParams(vmem_limit_bytes=4 << 20),
    )
    return run(first, second) if fresh else run(first, second, out)


def turn_kernel(pieces, count, signal, *refs):
    others, outs, copied = refs[:count], refs[count : count + pieces], refs[count + pieces : 2 * count + pieces]
    held, sems = refs[2 * count + pieces :]
    place = lax.axis_index("seq") // 2
    share = outs[0].shape[0]
    order = [*range(1, pieces), 0]
    starts = [pl.multiple_of(lax.bitwise_xor(place, k) * share, share) for k in order]
    sources = [signal.at[:, pl.ds(at, share)] for at in starts]
    copies = fetch([*sources, *others], [*(held.at[n] for n in range(pieces)), *copied], sems)
    for n, k in enumerate(order):
        copies[n].wait()
        outs[k][...] = held[n].T
    for copy in copies[pieces:]:
        copy.wait()


def call(kernel, outs, *args, scratch=(), flops=0, grant=12, hbm=()):
    spaces = [pltpu.HBM if n in hbm else VMEM for n in range(len(args))]
    run = pl.pallas_call(
        kernel,
        out_shape=outs,
        in_specs=[pl.BlockSpec(memory_space=space) for space in spaces],
        out_specs=jax.tree.map(lambda _: pl.BlockSpec(memory_space=VMEM), outs),
        scratch_shapes=list(scratch),
        cost_estimate=pl.CostEstimate(flops=flops, bytes_accessed=0, transcendentals=0),
        compiler_params=pltpu.CompilerParams(vmem_limit_bytes=grant << 20),
    )
    args = [
        pltpu.with_memory_space_constraint(arg, pltpu.HBM) if n in hbm else arg
        for n, arg in enumerate(args)
    ]
    return run(*args)


def shape(dims, dtype=BF16):
    return jax.ShapeDtypeStruct(dims, dtype)


def flip(x, axis, by):
    size = lax.axis_size(axis)
    return lax.ppermute(x, axis, [(i, i ^ by) for i in range(size)])


def spread(signal, gate, skip, w_first, b_first, freq, w_mid, w_last, rate, out_w):
    length_local, channels = signal.shape
    ranks, heads = lax.axis_size("seq"), lax.axis_size("head")
    pieces = ranks // 2
    share = channels // pieces
    per = length_local // BLOCK
    blocks = ranks * per
    taps = K // BLOCK
    half = length_local // 2
    width = out_w.shape[1] // heads
    row = lambda v: v.reshape(1, -1)

    forward_high, forward_low = split(forward_table())
    block_table = np.concatenate([forward_high[:BLOCK], forward_low[:BLOCK]], 0)
    back_table = np.concatenate(split(backward_table()), 1)
    operands = (
        jnp.asarray(feature_table()),
        w_first,
        row(b_first),
        row(freq),
        w_mid,
        w_last,
        row(rate),
    )
    piece = shape((share, length_local))
    turned = call(
        functools.partial(turn_kernel, pieces, len(operands)),
        (piece,) * pieces + tuple(shape(v.shape, v.dtype) for v in operands),
        signal,
        *operands,
        scratch=[
            pltpu.VMEM((pieces, length_local, share), BF16),
            pltpu.SemaphoreType.DMA((pieces + len(operands),)),
        ],
        hbm=range(1 + len(operands)),
    )
    own, operands = turned[:pieces], turned[pieces:]
    near = [flip(own[k], "seq", 2 * k) if k else own[0] for k in range(pieces)]
    beside = [flip(near[k], "seq", 1) for k in range(pieces)]

    hidden = call(
        hidden_kernel,
        shape((3 * w_mid.shape[1], K)),
        *operands[:5],
        scratch=[pltpu.VMEM((operands[0].shape[0] // 2 * 3, w_first.shape[1]), BF16)],
        flops=1_000_000_000,
    )
    filt = call(
        filter_kernel,
        shape((taps, share, 2 * BLOCK), F32),
        hidden,
        *operands[5:],
        forward_high,
        forward_low,
        flops=2_000_000_000,
    )
    other_w = flip(out_w, "head", 1)
    sums = shape((blocks // 2, share, 2 * BLOCK), F32)
    early = call(
        functools.partial(own_kernel, pieces),
        sums,
        filt,
        block_table,
        *near,
        scratch=[pltpu.VMEM(sums.shape, F32)],
        flops=1_000_000_000,
    )
    convs = call(
        functools.partial(conv_kernel, pieces),
        (piece,) * pieces,
        filt,
        block_table,
        back_table,
        early,
        *beside,
        scratch=[
            pltpu.VMEM((per + blocks // 2, share, 2 * BLOCK), F32),
            pltpu.VMEM(sums.shape, F32),
            pltpu.VMEM((blocks // 2, share, BLOCK), BF16),
        ],
        flops=3_000_000_000,
    )

    convs = [flip(conv, "seq", 2 * k) if k else conv for k, conv in enumerate(convs)]
    mixed = shape((half, channels))
    keep, send = call(
        functools.partial(mix_kernel, pieces),
        (mixed, mixed),
        signal,
        gate,
        row(skip),
        *convs,
        scratch=[pltpu.VMEM((pieces, share, length_local), BF16)],
        flops=500_000_000,
    )
    received = flip(send, "head", 1)
    wide = shape((half, width), F32)
    flips = (2, 3, 1, 0)
    sums = call(functools.partial(project_kernel, flips), (wide,) * 4, keep, out_w, flops=500_000_000)

    def project(which, dtype):
        return call(
            functools.partial(add_kernel, [flips[n] for n in which]),
            (shape((half, width), dtype),) * len(which),
            received,
            other_w,
            *(sums[n] for n in which),
            flops=500_000_000,
        )

    (a,) = project((0,), BF16)
    a = flip(a, "head", 2)
    (b,) = project((1,), BF16)
    b = flip(b, "head", 3)
    c, here = project((2, 3), F32)
    c = flip(c, "head", 1)
    out = add_half(0, shape((length_local, width)), here, a)
    return add_half(1, out, c, b)


def shifted(x, axis, by):
    size = lax.axis_size(axis)
    pairs = [(i, i + by) for i in range(size) if 0 <= i + by < size]
    return lax.ppermute(x, axis, pairs)


def make_filter(w_first, b_first, freq, w_mid, w_last, rate, count):
    position = jnp.arange(count).astype(jnp.float32)
    bands = jnp.arange(1, BANDS + 1).astype(jnp.float32)
    angles = 2.0 * math.pi * position[:, None] * bands[None, :] / K
    features = jnp.concatenate([position[:, None] / K, jnp.cos(angles), jnp.sin(angles)], 1)
    first = jnp.sin(freq * (jnp.dot(features, w_first, precision=HIGHEST) + b_first))
    second = jnp.sin(freq * jnp.dot(first, w_mid, precision=HIGHEST))
    raw = jnp.dot(second, w_last, precision=HIGHEST)
    return (raw * jnp.exp(-rate[None, :] * position[:, None])).astype(jnp.bfloat16)


def transform_tables(block):
    doubled = 2 * block
    taps = jnp.arange(block)
    freqs = jnp.arange(block)
    outputs = jnp.arange(doubled)
    scale_angle = 2.0 * math.pi / doubled
    phase = (freqs[:, None] * taps[None, :] % doubled).astype(jnp.float32) * scale_angle
    alternate = (1 - 2 * (taps % 2)).astype(jnp.float32)
    forward_real = jnp.cos(phase)
    forward_imag = jnp.where(freqs[:, None] == 0, alternate[None, :], -jnp.sin(phase))
    phase_back = (outputs[:, None] * freqs[None, :] % doubled).astype(jnp.float32) * scale_angle
    alternate_back = (1 - 2 * (outputs % 2)).astype(jnp.float32)
    weights = jnp.where(freqs == 0, 1.0, 2.0).astype(jnp.float32)
    back_real = weights[None, :] * jnp.cos(phase_back) / doubled
    back_imag = (
        jnp.where(freqs[None, :] == 0, alternate_back[:, None], -2.0 * jnp.sin(phase_back))
        / doubled
    )
    return (forward_real, forward_imag, back_real, back_imag)


def long_convolve(padded, filt, length_local):
    channels = padded.shape[1]
    block = min(128, length_local)
    segments = K // block
    out_blocks = length_local // block
    in_blocks = padded.shape[0] // block
    forward_real, forward_imag, back_real, back_imag = transform_tables(block)
    values = padded.astype(jnp.float32).reshape(in_blocks, block, channels)
    kernels = filt.astype(jnp.float32).reshape(segments, block, channels)[::-1]
    spec_real = jnp.einsum("ft,ntc->nfc", forward_real, values, precision=HIGHEST)
    spec_imag = jnp.einsum("ft,ntc->nfc", forward_imag, values, precision=HIGHEST)
    kern_real = jnp.einsum("ft,ntc->nfc", forward_real, kernels, precision=HIGHEST)
    kern_imag = jnp.einsum("ft,ntc->nfc", forward_imag, kernels, precision=HIGHEST)
    upper = (jnp.arange(block) >= 1).astype(jnp.float32)[:, None]
    sums_real = []
    sums_imag = []
    for index in range(out_blocks + 1):
        window_real = spec_real[index : index + segments]
        window_imag = spec_imag[index : index + segments]
        both_imag = kern_imag * window_imag
        sums_real.append(jnp.sum(kern_real * window_real - upper * both_imag, 0))
        cross = kern_real * window_imag + kern_imag * window_real
        sums_imag.append(jnp.sum(upper * cross + (1.0 - upper) * both_imag, 0))
    total_real = jnp.stack(sums_real, 0)
    total_imag = jnp.stack(sums_imag, 0)
    pieces = jnp.einsum("tf,kfc->ktc", back_real, total_real, precision=HIGHEST)
    pieces = pieces + jnp.einsum("tf,kfc->ktc", back_imag, total_imag, precision=HIGHEST)
    joined = pieces[1:, :block] + pieces[:-1, block:]
    return joined.reshape(length_local, channels)


def halo(signal, gate, skip, w_first, b_first, freq, w_mid, w_last, rate, out_w):
    length_local, _ = signal.shape
    filt = make_filter(w_first, b_first, freq, w_mid, w_last, rate, K)
    reach = K // length_local
    earlier = [shifted(signal, "seq", step) for step in range(reach, 0, -1)]
    padded = jnp.concatenate(earlier + [signal], 0)
    conv = long_convolve(padded, filt, length_local)
    mixed = (gate.astype(jnp.float32) * (conv + skip[None, :] * signal.astype(jnp.float32))).astype(
        jnp.bfloat16
    )
    terms = jnp.dot(mixed, out_w, preferred_element_type=jnp.float32)
    result = lax.psum_scatter(terms, "head", scatter_dimension=1, tiled=True)
    return result.astype(jnp.bfloat16)


def local(signal, *rest):
    ranks, heads = lax.axis_size("seq"), lax.axis_size("head")
    length_local, channels = signal.shape
    small = ranks == 8 and ranks * length_local <= K and heads == 4 and length_local == 2 * BLOCK
    if small and channels == 128 * (ranks // 2):
        return spread(signal, *rest)
    return halo(signal, *rest)


def solution(mesh):
    placed = (
        P("seq", "head"),
        P("seq", "head"),
        P("head"),
        P(),
        P(),
        P(),
        P(),
        P(None, "head"),
        P("head"),
        P("head", None),
    )


    return jax.shard_map(
        local, mesh=mesh, in_specs=placed, out_specs=P("seq", "head"), check_vma=False
    )
```

```python
import functools
import math

import jax
import jax.numpy as jnp
import numpy as np
from jax import lax
from jax.experimental import pallas as pl
from jax.experimental.pallas import tpu as pltpu
from jax.sharding import PartitionSpec as P


K = 2048
BANDS = 16
BLOCK = 128
TILE = 16
VMEM = pltpu.MemorySpace.VMEM
BF16 = jnp.bfloat16
F32 = jnp.float32
HIGHEST = lax.Precision.HIGHEST


def feature_table():
    taps = np.arange(K, dtype=np.float64)
    bands = np.arange(1, BANDS + 1, dtype=np.float64)
    angles = 2.0 * np.pi * ((taps[None, :] * bands[:, None]) % K) / K
    features = np.concatenate([taps[None, :] / K, np.cos(angles), np.sin(angles)], 0)
    features = np.pad(features, ((0, -len(features) % TILE), (0, 0)))
    return np.concatenate(split(features), 0)


def split(table):
    table = np.asarray(table, np.float32)
    high = table.astype(BF16)
    low = (table - high.astype(np.float32)).astype(BF16)
    return high, low


def forward_table():
    size = 2 * BLOCK
    samples = np.arange(size)
    freqs = np.arange(BLOCK)
    phase = 2.0 * np.pi * ((samples[:, None] * freqs[None, :]) % size) / size
    real = np.cos(phase)
    imag = -np.sin(phase)
    imag[:, 0] = 1.0 - 2.0 * (samples % 2)
    return np.concatenate([real, imag], 1)


def backward_table():
    size = 2 * BLOCK
    samples = np.arange(BLOCK, size)
    freqs = np.arange(BLOCK)
    phase = 2.0 * np.pi * ((freqs[:, None] * samples[None, :]) % size) / size
    real = 2.0 * np.cos(phase)
    imag = -2.0 * np.sin(phase)
    real[0] = 1.0
    imag[0] = 1.0 - 2.0 * (samples % 2)
    return np.concatenate([real, imag], 0) / size


def dot(a, b):
    return jnp.dot(a, b, preferred_element_type=F32)


SINE = (6.283182621, -41.34142303, 81.59618378, -76.58010101, 41.20539856, -12.27126789)


def sine(turns):
    r = turns - jnp.round(turns)
    s = r * r
    p = SINE[-1] * s + SINE[-2]
    for value in SINE[-3::-1]:
        p = p * s + value
    return p * r


def column(row):
    n = row.shape[1]
    square = (n, n)
    diagonal = lax.broadcasted_iota(jnp.int32, square, 0) == lax.broadcasted_iota(jnp.int32, square, 1)
    return jnp.sum(jnp.where(diagonal, jnp.broadcast_to(row, square), 0.0), 1, keepdims=True)


def parts_of(x):
    high = x.astype(BF16)
    return high, (x - high.astype(F32)).astype(BF16)


def dot_first(a, b):
    return lax.dot_general(a, b, (((0,), (0,)), ((), ())), preferred_element_type=F32)


def stack_left(x):
    high, low = parts_of(x)
    return jnp.concatenate([high, high, low], 0)


def stack_right(x):
    high, low = parts_of(x)
    return jnp.concatenate([high, low, high], 0)


def fetch(sources, targets, sems):
    copies = [
        pltpu.make_async_copy(source, target, sems.at[n])
        for n, (source, target) in enumerate(zip(sources, targets))
    ]
    for copy in copies:
        copy.start()
    return copies


def hidden_kernel(feat, w_first, bias, freq, w_mid, out, left):
    turns = column(freq[...] * (0.5 / math.pi))
    high, low = parts_of(w_first[...])
    count = high.shape[0]
    rows = left.shape[0] // 3
    left[...] = jnp.zeros(left.shape, BF16)
    for n, part in enumerate((high, high, low)):
        left[n * rows : n * rows + count, :] = part
    features = jnp.concatenate([feat[...], feat[:rows]], 0)
    first = sine(turns * (dot_first(left[...], features) + column(bias[...])))
    second = sine(turns * dot_first(stack_left(w_mid[...]), stack_right(first)))
    out[...] = stack_right(second)


def filter_kernel(hidden, w_last, rate, table_high, table_low, out):
    share = out.shape[1]
    own = pl.ds(pl.multiple_of((lax.axis_index("seq") // 2) * share, share), share)
    raw = dot_first(stack_left(w_last[:, own]), hidden[...])
    rates = column(rate[:, own])
    lane = lax.broadcasted_iota(jnp.int32, (1, BLOCK), 1).astype(F32)
    decay, step = jnp.exp(-rates * lane), jnp.exp(-rates * float(BLOCK))
    before = [jnp.zeros((share, BLOCK), BF16)]
    for j in range(out.shape[0]):
        before.append((raw[:, j * BLOCK : (j + 1) * BLOCK] * decay).astype(BF16))
        decay = decay * step
    window = jnp.concatenate([jnp.concatenate(before[:-1], 0), jnp.concatenate(before[1:], 0)], 1)
    out[...] = (dot(window, table_high[...]) + dot(window, table_low[...])).reshape(out.shape)


def spectra(pieces, spec, first, flips, table):
    place = lax.axis_index("seq") // 2
    per = pieces[0].shape[1] // BLOCK
    for flip, piece in zip(flips, pieces):
        at = (lax.bitwise_xor(place, flip) + first) * per
        for part in range(per):
            block = piece[:, part * BLOCK : (part + 1) * BLOCK]
            spec[at + part] = dot(jnp.concatenate([block, block], 1), table[...])


def products(filt, spec, places, per, shift, apart, done):
    taps = filt.shape[0]
    packed = lax.broadcasted_iota(jnp.int32, (8, BLOCK), 1) == 0

    def group(g, carry):
        at = pl.ds(pl.multiple_of(g * 8, 8), 8)

        def load(ref, index):
            real, imag = ref[index, at, :BLOCK], ref[index, at, BLOCK:]
            return real, imag, real + imag

        for place in range(places):
            sums = [None] * per
            for d in range(place + 1):
                held = [load(spec, (place - d + shift) * per + r) for r in range(per)]
                windows = {}
                for q in range(per):
                    for r in range(per):
                        j = 2 * per * d + apart + q - r
                        if 0 <= j < taps:
                            if j not in windows:
                                windows[j] = load(filt, j)
                            terms = tuple(x * f for x, f in zip(held[r], windows[j]))
                            sums[q] = terms if sums[q] is None else tuple(s + t for s, t in zip(sums[q], terms))
            for q, (real, imag, both) in enumerate(sums):
                done(
                    per * place + q,
                    at,
                    real - jnp.where(packed, 0.0, imag),
                    jnp.where(packed, imag, both - real - imag),
                )
        return carry

    lax.fori_loop(0, spec.shape[1] // 8, group, 0)


def own_kernel(pieces, filt, table, *refs):
    ins, out, spec = refs[:pieces], refs[pieces], refs[pieces + 1]
    per = ins[0].shape[1] // BLOCK
    spectra(ins, spec, 0, range(pieces), table)

    def done(block, at, real, imag):
        out[block, at, :BLOCK] = real
        out[block, at, BLOCK:] = imag

    products(filt, spec, pieces, per, 0, 0, done)


def side_kernel(table, *refs):
    ins, spec = refs[:-1], refs[-1]
    per = ins[0].shape[1] // BLOCK
    spec[0:per] = jnp.zeros((per,) + spec.shape[1:], F32)
    spectra(ins, spec, 1, range(len(ins)), table)


def conv_kernel(pieces, filt, table, back, own, spec, last, *refs):
    outs, total, result = refs[:pieces], *refs[pieces + 1 :]
    me = lax.axis_index("seq")
    per = last.shape[1] // BLOCK
    spectra([last], spec, 1, [pieces - 1], table)

    def done(block, at, real, imag):
        total[block, at, :BLOCK] = own[block, at, :BLOCK] + real
        total[block, at, BLOCK:] = own[block, at, BLOCK:] + imag

    products(filt, spec, pieces, per, lax.rem(me, 2), per, done)
    high, low = parts_of(total[...].reshape(-1, 2 * BLOCK))
    conv = dot(high, back[...])
    conv = conv[:, :BLOCK] + conv[:, BLOCK:] + dot(low, back[:, :BLOCK])
    result[...] = conv.astype(BF16).reshape(result.shape)
    for k, out in enumerate(outs):
        at = lax.bitwise_xor(me // 2, k) * per
        out[...] = jnp.concatenate([result[at + part] for part in range(per)], 1)


def gated(part, signal, gate, skip, pieces, ordered):
    place = lax.axis_index("seq") // 2
    half = signal.shape[0] // 2
    at = pl.ds(pl.multiple_of(part * half, half), half)
    for k, piece in enumerate(pieces):
        ordered[lax.bitwise_xor(place, k)] = piece[:, at]
    turned = ordered[...].reshape(-1, half).T.astype(F32)
    return (gate[at, :].astype(F32) * (turned + skip[...] * signal[at, :].astype(F32))).astype(BF16)


def mix_kernel(pieces, signal, gate, skip, *refs):
    ins, (out, ordered) = refs[:pieces], refs[pieces:]
    core = lax.rem(lax.axis_index("head"), 2)
    out[...] = gated(1 - core, signal, gate, skip, ins, ordered)


def project_kernel(pieces, flips, weights, signal, gate, skip, *refs):
    ins, outs, ordered = refs[:pieces], refs[pieces:-1], refs[-1]
    head = lax.axis_index("head")
    own = gated(lax.rem(head, 2), signal, gate, skip, ins, ordered)
    width = outs[0].shape[1]
    for flip, out in zip(flips, outs):
        columns = pl.ds(pl.multiple_of(lax.bitwise_xor(head, flip) * width, width), width)
        out[...] = dot(own, weights[:, columns])


def add_kernel(flips, other, weights, *refs):
    sums, outs = refs[: len(flips)], refs[len(flips) :]
    head = lax.axis_index("head")
    width = outs[0].shape[1]
    for flip, total, out in zip(flips, sums, outs):
        columns = pl.ds(pl.multiple_of(lax.bitwise_xor(head, flip) * width, width), width)
        out[...] = (total[...] + dot(other[...], weights[:, columns])).astype(out.dtype)


def sum_kernel(other_half, first, second, *refs):
    out, held, sem = refs[-3:]
    half = held.shape[0]
    part = lax.bitwise_xor(lax.rem(lax.axis_index("head"), 2), other_half)
    held[...] = (first[...].astype(F32) + second[...].astype(F32)).astype(BF16)
    rows = pl.ds(pl.multiple_of(part * half, half), half)
    copy = pltpu.make_async_copy(held, out.at[rows, :], sem)
    copy.start()
    copy.wait()


def add_half(other_half, out, first, second):
    fresh = isinstance(out, jax.ShapeDtypeStruct)
    half, width = first.shape
    run = pl.pallas_call(
        functools.partial(sum_kernel, other_half),
        out_shape=shape(out.shape),
        in_specs=[pl.BlockSpec(memory_space=VMEM)] * 2 + [pl.BlockSpec(memory_space=pltpu.HBM)] * (not fresh),
        out_specs=pl.BlockSpec(memory_space=pltpu.HBM),
        scratch_shapes=[pltpu.VMEM((half, width), BF16), pltpu.SemaphoreType.DMA(())],
        input_output_aliases={} if fresh else {2: 0},
        cost_estimate=pl.CostEstimate(flops=100_000_000, bytes_accessed=0, transcendentals=0),
        compiler_params=pltpu.CompilerParams(vmem_limit_bytes=4 << 20),
    )
    return run(first, second) if fresh else run(first, second, out)


def turn_kernel(pieces, count, signal, *refs):
    others, outs, copied = refs[:count], refs[count : count + pieces], refs[count + pieces : 2 * count + pieces]
    held, sems = refs[2 * count + pieces :]
    place = lax.axis_index("seq") // 2
    share = outs[0].shape[0]
    order = [*range(1, pieces), 0]
    starts = [pl.multiple_of(lax.bitwise_xor(place, k) * share, share) for k in order]
    sources = [signal.at[:, pl.ds(at, share)] for at in starts]
    copies = fetch([*sources, *others], [*(held.at[n] for n in range(pieces)), *copied], sems)
    for n, k in enumerate(order):
        copies[n].wait()
        outs[k][...] = held[n].T
    for copy in copies[pieces:]:
        copy.wait()


def call(kernel, outs, *args, scratch=(), flops=0, grant=12, hbm=(), aliases=None):
    spaces = [pltpu.HBM if n in hbm else VMEM for n in range(len(args))]
    run = pl.pallas_call(
        kernel,
        out_shape=outs,
        in_specs=[pl.BlockSpec(memory_space=space) for space in spaces],
        out_specs=jax.tree.map(lambda _: pl.BlockSpec(memory_space=VMEM), outs),
        scratch_shapes=list(scratch),
        input_output_aliases=aliases or {},
        cost_estimate=pl.CostEstimate(flops=flops, bytes_accessed=0, transcendentals=0),
        compiler_params=pltpu.CompilerParams(vmem_limit_bytes=grant << 20),
    )
    args = [
        pltpu.with_memory_space_constraint(arg, pltpu.HBM) if n in hbm else arg
        for n, arg in enumerate(args)
    ]
    return run(*args)


def shape(dims, dtype=BF16):
    return jax.ShapeDtypeStruct(dims, dtype)


def flip(x, axis, by):
    size = lax.axis_size(axis)
    return lax.ppermute(x, axis, [(i, i ^ by) for i in range(size)])


def spread(signal, gate, skip, w_first, b_first, freq, w_mid, w_last, rate, out_w):
    length_local, channels = signal.shape
    ranks, heads = lax.axis_size("seq"), lax.axis_size("head")
    pieces = ranks // 2
    share = channels // pieces
    per = length_local // BLOCK
    blocks = ranks * per
    taps = K // BLOCK
    half = length_local // 2
    width = out_w.shape[1] // heads
    row = lambda v: v.reshape(1, -1)

    forward_high, forward_low = split(forward_table())
    block_table = np.concatenate([forward_high[:BLOCK], forward_low[:BLOCK]], 0)
    back_table = np.concatenate(split(backward_table()), 1)
    operands = (
        jnp.asarray(feature_table()),
        w_first,
        row(b_first),
        row(freq),
        w_mid,
        w_last,
        row(rate),
    )
    piece = shape((share, length_local))
    turned = call(
        functools.partial(turn_kernel, pieces, len(operands)),
        (piece,) * pieces + tuple(shape(v.shape, v.dtype) for v in operands),
        signal,
        *operands,
        scratch=[
            pltpu.VMEM((pieces, length_local, share), BF16),
            pltpu.SemaphoreType.DMA((pieces + len(operands),)),
        ],
        hbm=range(1 + len(operands)),
    )
    own, operands = turned[:pieces], turned[pieces:]
    near = [flip(own[k], "seq", 2 * k) if k else own[0] for k in range(pieces)]
    beside = [flip(near[k], "seq", 1) for k in range(pieces)]

    hidden = call(
        hidden_kernel,
        shape((3 * w_mid.shape[1], K)),
        *operands[:5],
        scratch=[pltpu.VMEM((operands[0].shape[0] // 2 * 3, w_first.shape[1]), BF16)],
        flops=1_000_000_000,
    )
    filt = call(
        filter_kernel,
        shape((taps, share, 2 * BLOCK), F32),
        hidden,
        *operands[5:],
        forward_high,
        forward_low,
        flops=2_000_000_000,
    )
    other_w = flip(out_w, "head", 1)
    sums = shape((blocks // 2, share, 2 * BLOCK), F32)
    early = call(
        functools.partial(own_kernel, pieces),
        sums,
        filt,
        block_table,
        *near,
        scratch=[pltpu.VMEM(sums.shape, F32)],
        flops=1_000_000_000,
    )
    side = shape((per + blocks // 2, share, 2 * BLOCK), F32)
    first = call(side_kernel, side, block_table, *beside[:-1], flops=500_000_000)
    *convs, _ = call(
        functools.partial(conv_kernel, pieces),
        (piece,) * pieces + (side,),
        filt,
        block_table,
        back_table,
        early,
        first,
        beside[-1],
        scratch=[
            pltpu.VMEM(sums.shape, F32),
            pltpu.VMEM((blocks // 2, share, BLOCK), BF16),
        ],
        flops=3_000_000_000,
        aliases={4: pieces},
    )

    convs = [flip(conv, "seq", 2 * k) if k else conv for k, conv in enumerate(convs)]
    gating = (signal, gate, row(skip), *convs)
    ordered = pltpu.VMEM((pieces, share, half), BF16)
    send = call(
        functools.partial(mix_kernel, pieces), shape((half, channels)), *gating, scratch=[ordered], flops=500_000_000
    )
    received = flip(send, "head", 1)
    wide = shape((half, width), F32)
    flips = (2, 3, 1, 0)
    sums = call(
        functools.partial(project_kernel, pieces, flips),
        (wide,) * 4,
        out_w,
        *gating,
        scratch=[ordered],
        flops=500_000_000,
    )

    def project(which, dtype):
        return call(
            functools.partial(add_kernel, [flips[n] for n in which]),
            (shape((half, width), dtype),) * len(which),
            received,
            other_w,
            *(sums[n] for n in which),
            flops=500_000_000,
        )

    (a,) = project((0,), BF16)
    a = flip(a, "head", 2)
    (b,) = project((1,), BF16)
    b = flip(b, "head", 3)
    c, here = project((2, 3), F32)
    c = flip(c, "head", 1)
    out = add_half(0, shape((length_local, width)), here, a)
    return add_half(1, out, c, b)


def shifted(x, axis, by):
    size = lax.axis_size(axis)
    pairs = [(i, i + by) for i in range(size) if 0 <= i + by < size]
    return lax.ppermute(x, axis, pairs)


def make_filter(w_first, b_first, freq, w_mid, w_last, rate, count):
    position = jnp.arange(count).astype(jnp.float32)
    bands = jnp.arange(1, BANDS + 1).astype(jnp.float32)
    angles = 2.0 * math.pi * position[:, None] * bands[None, :] / K
    features = jnp.concatenate([position[:, None] / K, jnp.cos(angles), jnp.sin(angles)], 1)
    first = jnp.sin(freq * (jnp.dot(features, w_first, precision=HIGHEST) + b_first))
    second = jnp.sin(freq * jnp.dot(first, w_mid, precision=HIGHEST))
    raw = jnp.dot(second, w_last, precision=HIGHEST)
    return (raw * jnp.exp(-rate[None, :] * position[:, None])).astype(jnp.bfloat16)


def transform_tables(block):
    doubled = 2 * block
    taps = jnp.arange(block)
    freqs = jnp.arange(block)
    outputs = jnp.arange(doubled)
    scale_angle = 2.0 * math.pi / doubled
    phase = (freqs[:, None] * taps[None, :] % doubled).astype(jnp.float32) * scale_angle
    alternate = (1 - 2 * (taps % 2)).astype(jnp.float32)
    forward_real = jnp.cos(phase)
    forward_imag = jnp.where(freqs[:, None] == 0, alternate[None, :], -jnp.sin(phase))
    phase_back = (outputs[:, None] * freqs[None, :] % doubled).astype(jnp.float32) * scale_angle
    alternate_back = (1 - 2 * (outputs % 2)).astype(jnp.float32)
    weights = jnp.where(freqs == 0, 1.0, 2.0).astype(jnp.float32)
    back_real = weights[None, :] * jnp.cos(phase_back) / doubled
    back_imag = (
        jnp.where(freqs[None, :] == 0, alternate_back[:, None], -2.0 * jnp.sin(phase_back))
        / doubled
    )
    return (forward_real, forward_imag, back_real, back_imag)


def long_convolve(padded, filt, length_local):
    channels = padded.shape[1]
    block = min(128, length_local)
    segments = K // block
    out_blocks = length_local // block
    in_blocks = padded.shape[0] // block
    forward_real, forward_imag, back_real, back_imag = transform_tables(block)
    values = padded.astype(jnp.float32).reshape(in_blocks, block, channels)
    kernels = filt.astype(jnp.float32).reshape(segments, block, channels)[::-1]
    spec_real = jnp.einsum("ft,ntc->nfc", forward_real, values, precision=HIGHEST)
    spec_imag = jnp.einsum("ft,ntc->nfc", forward_imag, values, precision=HIGHEST)
    kern_real = jnp.einsum("ft,ntc->nfc", forward_real, kernels, precision=HIGHEST)
    kern_imag = jnp.einsum("ft,ntc->nfc", forward_imag, kernels, precision=HIGHEST)
    upper = (jnp.arange(block) >= 1).astype(jnp.float32)[:, None]
    sums_real = []
    sums_imag = []
    for index in range(out_blocks + 1):
        window_real = spec_real[index : index + segments]
        window_imag = spec_imag[index : index + segments]
        both_imag = kern_imag * window_imag
        sums_real.append(jnp.sum(kern_real * window_real - upper * both_imag, 0))
        cross = kern_real * window_imag + kern_imag * window_real
        sums_imag.append(jnp.sum(upper * cross + (1.0 - upper) * both_imag, 0))
    total_real = jnp.stack(sums_real, 0)
    total_imag = jnp.stack(sums_imag, 0)
    pieces = jnp.einsum("tf,kfc->ktc", back_real, total_real, precision=HIGHEST)
    pieces = pieces + jnp.einsum("tf,kfc->ktc", back_imag, total_imag, precision=HIGHEST)
    joined = pieces[1:, :block] + pieces[:-1, block:]
    return joined.reshape(length_local, channels)


def halo(signal, gate, skip, w_first, b_first, freq, w_mid, w_last, rate, out_w):
    length_local, _ = signal.shape
    filt = make_filter(w_first, b_first, freq, w_mid, w_last, rate, K)
    reach = K // length_local
    earlier = [shifted(signal, "seq", step) for step in range(reach, 0, -1)]
    padded = jnp.concatenate(earlier + [signal], 0)
    conv = long_convolve(padded, filt, length_local)
    mixed = (gate.astype(jnp.float32) * (conv + skip[None, :] * signal.astype(jnp.float32))).astype(
        jnp.bfloat16
    )
    terms = jnp.dot(mixed, out_w, preferred_element_type=jnp.float32)
    result = lax.psum_scatter(terms, "head", scatter_dimension=1, tiled=True)
    return result.astype(jnp.bfloat16)


def local(signal, *rest):
    ranks, heads = lax.axis_size("seq"), lax.axis_size("head")
    length_local, channels = signal.shape
    small = ranks == 8 and ranks * length_local <= K and heads == 4 and length_local == 2 * BLOCK
    if small and channels == 128 * (ranks // 2):
        return spread(signal, *rest)
    return halo(signal, *rest)


def solution(mesh):
    placed = (
        P("seq", "head"),
        P("seq", "head"),
        P("head"),
        P(),
        P(),
        P(),
        P(),
        P(None, "head"),
        P("head"),
        P("head", None),
    )


    return jax.shard_map(
        local, mesh=mesh, in_specs=placed, out_specs=P("seq", "head"), check_vma=False
    )
```
